256 devices in a mesh: grp: 8 (over x, core), dp: 32 (over y, z).
Axes of the slice: x: 4, y: 4, z: 8, core: 2. Of those that a mesh axis runs over, the one named last changes fastest.
Arguments:
- chosen_ids: int32 [256, 512], P(('grp', 'dp')), may hold values from 0 to 128255, as said below
- rejected_ids: int32 [256, 512], P(('grp', 'dp')), may hold values from 0 to 128255, as said below
- chosen_len: int32 [256], P(('grp', 'dp')), may hold values from 64 to 256
- rejected_len: int32 [256], P(('grp', 'dp')), may hold values from 64 to 256
- chosen_logp: float32 [256, 512], P(('grp', 'dp')), may hold values from -0.3 to -0.01
- rejected_logp: float32 [256, 512], P(('grp', 'dp')), may hold values from -0.3 to -0.01
- ref_logp: float32 [2, 256], P(None, ('grp', 'dp')), may hold values from -40 to -10
- chosen_grads: bfloat16 [256, 512, 4096], P(('grp', 'dp')), may hold values from -48 to 48
- rejected_grads: bfloat16 [256, 512, 4096], P(('grp', 'dp')), may hold values from -48 to 48
Outputs:
- grad_table: bfloat16 [128256, 4096], P(('grp', 'dp'))
The draws below stay inside these ranges and needn't reach their ends.
Inputs may be any that keep to these rules, and one draw needn't show every extreme that they name: `chosen_ids`: vocabulary row v belongs to owner v // 501. The chosen and rejected tokens of one device's pairs together fall at most 6 times into one owner's rows; 16 owners drawn from the seed get exactly 6 of them from every device. `rejected_ids`: drawn together with chosen_ids under the same bound. The response is the last chosen_len[p] positions of the sequence. The response is the last rejected_len[p] positions of the sequence.
All inputs are finite; a program needn't handle non-finite values.
Results may differ from the reference program's by a relative error of at most 0.001.
The reference program's roundings to bfloat16 on the way count: a program that leaves them out, or rounds other values in their place, can miss the bound.
Values may be sent and summed in bfloat16 or wider, within the bound.
No kernel may reach another device: no remote copies, remote signals or barrier semaphores. Data moves between devices by JAX's collectives and lax.ppermute only.
A program may use at most 128 MiB of HBM per device.

```python
import jax
import jax.numpy as jnp
from jax import lax

D = 4096
VOCAB = 128256
SEQ = 512
PAIRS_DEV = 1
HOT = 16
OWNERS = 256
ROWS_OWN = 501
CAP = 6
PAIRS = 256
DEVICES = 256


def token_table(key):
    base = jax.random.fold_in(key, 7)
    hot_list = jax.random.permutation(jax.random.fold_in(base, 1), OWNERS)[:HOT]
    hot_flag = jnp.zeros((OWNERS,), jnp.int32).at[hot_list].set(1)
    slot_total = OWNERS * CAP
    block_size = 2 * PAIRS_DEV * SEQ
    slot_owner = jnp.arange(slot_total, dtype=jnp.int32) // CAP

    def one_device(device_index):
        device_key = jax.random.fold_in(base, 100 + device_index)
        score_key, shuffle_key, row_key = jax.random.split(device_key, 3)
        scores = jax.random.randint(score_key, (slot_total,), 0, 65536) - hot_flag[slot_owner] * 131072
        picked = jnp.argsort(scores, stable=True)[:block_size]
        owner_pick = slot_owner[picked]
        owner_pick = owner_pick[jax.random.permutation(shuffle_key, block_size)]
        row_pick = jax.random.randint(row_key, (block_size,), 0, ROWS_OWN)
        return (owner_pick * ROWS_OWN + row_pick).astype(jnp.int32)
    every_block = jax.vmap(one_device)(jnp.arange(DEVICES))
    half = PAIRS_DEV * SEQ
    chosen = every_block[:, :half].reshape(PAIRS, SEQ)
    rejected = every_block[:, half:].reshape(PAIRS, SEQ)
    return (chosen, rejected)


def draw_chosen_ids(key, part):
    return token_table(key)[0]


def draw_rejected_ids(key, part):
    return token_table(key)[1]


def plant(drawn, own_key, least, largest):
    longest = drawn.shape.index(max(drawn.shape))
    spots = []
    for shift in (0, 1):
        where = [jax.random.randint(jax.random.fold_in(own_key, axis), (), 0, length) for axis, length in enumerate(drawn.shape)]
        where[longest] = (where[longest] + shift) % drawn.shape[longest]
        spots.append(tuple(where))
    return drawn.at[spots[0]].set(least).at[spots[1]].set(largest)


def shard_levels(key, dims, cuts, least, high):
    def one(dim, blocks):
        heights = jax.random.uniform(jax.random.fold_in(jax.random.fold_in(key, 6), dim), (blocks,), jnp.float32, least / len(cuts), high / len(cuts))
        return jnp.repeat(jnp.exp(heights), dims[dim] // blocks).reshape((-1,) + (1,) * (len(dims) - dim - 1))

    loudness = one(*cuts[0])
    for cut in cuts[1:]:
        loudness = loudness * one(*cut)
    return loudness


def gaussian(key, dims, width, reach, cuts=(), kind=jnp.bfloat16):
    drawn = jax.random.normal(key, dims, jnp.float32) * width
    if len(cuts) > 0:
        drawn = shard_levels(key, dims, cuts, -0.22, 0.18) * drawn
    return jnp.clip(drawn, min=-reach, max=reach).astype(kind)


def setup_inputs(seed: int = 0) -> dict:
    splits = jax.random.split(jax.random.key(seed), 10)
    chosen_ids = draw_chosen_ids(jax.random.fold_in(splits[9], 71), 0)
    rejected_ids = draw_rejected_ids(jax.random.fold_in(splits[9], 71), 0)
    chosen_len = plant(jax.random.randint(splits[2], (PAIRS,), SEQ // 8, SEQ // 2 + 1), jax.random.fold_in(splits[2], 1), SEQ // 8, (SEQ // 2 + 1) - 1).astype(jnp.int32)
    rejected_len = plant(jax.random.randint(splits[3], (PAIRS,), SEQ // 8, SEQ // 2 + 1), jax.random.fold_in(splits[3], 1), SEQ // 8, (SEQ // 2 + 1) - 1).astype(jnp.int32)
    chosen_logp = jnp.clip(-0.3 + 0.29000001 * jax.random.uniform(splits[4], (PAIRS, SEQ), jnp.float32) ** shard_levels(splits[4], (PAIRS, SEQ), ((0, 256),), -0.2, 0.2), -0.3, -0.01)
    rejected_logp = jnp.clip(-0.3 + 0.29000001 * jax.random.uniform(splits[5], (PAIRS, SEQ), jnp.float32) ** shard_levels(splits[5], (PAIRS, SEQ), ((0, 256),), -0.2, 0.2), -0.3, -0.01)
    ref_logp = jnp.clip(-40.0 + 30.0 * jax.random.uniform(splits[6], (2, PAIRS), jnp.float32) ** shard_levels(splits[6], (2, PAIRS), ((1, 256),), -0.2, 0.2), -40.0, -10.0)
    chosen_grads = gaussian(splits[7], (PAIRS, SEQ, D), 8.0, 48.0, ((0, 256),))
    rejected_grads = gaussian(splits[8], (PAIRS, SEQ, D), 8.0, 48.0, ((0, 256),))
    return dict(chosen_ids=chosen_ids, rejected_ids=rejected_ids, chosen_len=chosen_len, rejected_len=rejected_len, chosen_logp=chosen_logp, rejected_logp=rejected_logp, ref_logp=ref_logp, chosen_grads=chosen_grads, rejected_grads=rejected_grads)


beta_scale = 0.1


def reference(chosen_ids, rejected_ids, chosen_len, rejected_len, chosen_logp, rejected_logp, ref_logp, chosen_grads, rejected_grads):
    positions = jnp.arange(SEQ)
    chosen_mask = (positions[None, :] >= SEQ - chosen_len[:, None]).astype(jnp.float32)
    rejected_mask = (positions[None, :] >= SEQ - rejected_len[:, None]).astype(jnp.float32)
    chosen_policy = jnp.sum(chosen_mask * chosen_logp, axis=1)
    rejected_policy = jnp.sum(rejected_mask * rejected_logp, axis=1)
    margin = beta_scale * ((chosen_policy - ref_logp[0]) - (rejected_policy - ref_logp[1]))
    pair_weight = beta_scale * jax.nn.sigmoid(-margin)

    def add_pair(pair_index, grad_table):
        weight_now = lax.dynamic_index_in_dim(pair_weight, pair_index, 0, keepdims=False)
        chosen_rows = lax.dynamic_index_in_dim(chosen_grads, pair_index, 0, keepdims=False)
        rejected_rows = lax.dynamic_index_in_dim(rejected_grads, pair_index, 0, keepdims=False)
        chosen_rows = (-weight_now * chosen_rows.astype(jnp.float32)).astype(jnp.bfloat16)
        rejected_rows = (weight_now * rejected_rows.astype(jnp.float32)).astype(jnp.bfloat16)
        chosen_slots = lax.dynamic_index_in_dim(chosen_ids, pair_index, 0, keepdims=False)
        rejected_slots = lax.dynamic_index_in_dim(rejected_ids, pair_index, 0, keepdims=False)
        grad_table = grad_table.at[chosen_slots].add(chosen_rows.astype(jnp.float32))
        grad_table = grad_table.at[rejected_slots].add(rejected_rows.astype(jnp.float32))
        return grad_table

    grad_table = lax.fori_loop(0, PAIRS, add_pair, jnp.zeros((VOCAB, D), jnp.float32))
    return grad_table.astype(jnp.bfloat16)
```

```python
import functools

import jax
import jax.numpy as jnp
from jax import lax
from jax.experimental import pallas as pl
from jax.experimental.pallas import tpu as pltpu
from jax.sharding import PartitionSpec as P

VOCAB = 128256
BETA = 0.1
UNITS = 4
WIDTHS = (2048, 2048)
STEPS = 4


def owner_of(ids, row_count):
    return jnp.floor((ids.astype(jnp.float32) + 0.5) * (1.0 / row_count))


def slots_of(ids, row_count, capacity):
    owner = owner_of(ids, row_count)
    tokens = ids.shape[1]
    blocks = tokens // 128
    lower = lax.broadcasted_iota(jnp.int32, (128, 128), 0) < lax.broadcasted_iota(
        jnp.int32, (128, 128), 1
    )
    rows = [owner[:, 128 * b : 128 * b + 128] for b in range(blocks)]
    columns = [jnp.transpose(jnp.broadcast_to(r, (128, 128))) for r in rows]
    ranks = []
    for j in range(blocks):
        hits = jnp.where((columns[j] == rows[j]) & lower, 1.0, 0.0)
        for i in range(j):
            hits = hits + jnp.where(columns[i] == rows[j], 1.0, 0.0)
        ranks.append(jnp.sum(hits, axis=0, keepdims=True))
    rank = jnp.concatenate(ranks, axis=1)
    return (owner * capacity + rank).astype(jnp.int32)


def weight_of(clen, rlen, clogp, rlogp, ref):
    length = clogp.shape[1]
    positions = lax.broadcasted_iota(jnp.int32, (1, length), 1)
    chosen_mask = (positions >= length - clen[0]).astype(jnp.float32)
    rejected_mask = (positions >= length - rlen[0]).astype(jnp.float32)
    chosen = jnp.sum(chosen_mask * clogp[...], axis=1, keepdims=True)
    rejected = jnp.sum(rejected_mask * rlogp[...], axis=1, keepdims=True)
    margin = BETA * ((chosen - ref[0, 0]) - (rejected - ref[1, 0]))
    return BETA * (1.0 / (1.0 + jnp.exp(margin)))


def send_kernel(
    cid, rid, clen, rlen, clogp, rlogp, ref, cg, rg, out, slot, rows, wide, *, row_count, capacity
):
    step = pl.program_id(0)
    half = cg.shape[1]
    height = out.shape[0] // UNITS
    width = out.shape[1]

    @pl.when(step == 0)
    def _():
        ids = jnp.concatenate([cid[...], rid[...]], axis=1)
        slot[...] = slots_of(ids, row_count, capacity)
        weight = weight_of(clen, rlen, clogp, rlogp, ref)
        rows[:half] = (-weight * cg[0].astype(jnp.float32)).astype(jnp.bfloat16)
        rows[half:] = (weight * rg[0].astype(jnp.float32)).astype(jnp.bfloat16)

    place = lax.broadcasted_iota(jnp.int32, (height, 2 * half), 0) + step * height
    pick = jnp.where(place == slot[...], 1.0, 0.0).astype(jnp.bfloat16)
    moved = jnp.dot(pick, rows[...], preferred_element_type=jnp.float32)
    for lane in range(width // 128):
        for u in range(UNITS):
            first = u * width + lane * 128
            wide[lane, pl.ds(u, height, stride=UNITS), :] = moved[:, first : first + 128]
        out[:, lane * 128 : lane * 128 + 128] = wide[lane].astype(jnp.bfloat16)


def label_kernel(cid, rid, out, *, row_count, capacity):
    ids = jnp.concatenate([cid[...], rid[...]], axis=1)
    slot = slots_of(ids, row_count, capacity)
    row = ids - owner_of(ids, row_count).astype(jnp.int32) * row_count
    total = out.shape[0]
    for b in range(0, total, 128):
        place = lax.broadcasted_iota(jnp.int32, (128, ids.shape[1]), 0) + b
        found = jnp.where(place == slot, row - row_count, 0)
        out[b : b + 128] = jnp.sum(found, axis=1, keepdims=True) + row_count


def receive_kernel(label, arrived, *refs):
    out, total, wide = refs[-3:]
    step = pl.program_id(0)
    height = arrived.shape[0] // UNITS

    @pl.when(step == 0)
    def _():
        total[...] = jnp.zeros_like(total)

    lanes = arrived.shape[1] // 128
    for lane in range(lanes):
        wide[lane] = arrived[:, lane * 128 : lane * 128 + 128].astype(jnp.float32)
    pieces = [
        wide[lane, pl.ds(u, height, stride=UNITS), :].astype(jnp.bfloat16)
        for u in range(UNITS)
        for lane in range(lanes)
    ]
    place = lax.broadcasted_iota(jnp.int32, (total.shape[0], height), 0)
    pick = jnp.where(place == label[...], 1.0, 0.0).astype(jnp.bfloat16)
    total[...] += jnp.dot(
        pick, jnp.concatenate(pieces, axis=1), preferred_element_type=jnp.float32
    )

    @pl.when(step == pl.num_programs(0) - 1)
    def _():
        out[...] = total[: out.shape[0]].astype(jnp.bfloat16)


def local(
    chosen_ids,
    rejected_ids,
    chosen_len,
    rejected_len,
    chosen_logp,
    rejected_logp,
    ref_logp,
    chosen_grads,
    rejected_grads,
):
    pair_count, length = chosen_ids.shape
    features = chosen_grads.shape[2]
    owners = lax.axis_size("grp") * lax.axis_size("dp")
    row_count = VOCAB // owners
    capacity = max(2, 3 * pair_count * length // owners)
    slots = owners * capacity
    axes = ("grp", "dp")
    smem = pl.BlockSpec(memory_space=pltpu.SMEM)
    padded = (row_count + 15) // 16 * 16
    sizes = dict(row_count=row_count, capacity=capacity)

    def whole(*shape):
        return pl.BlockSpec(shape, lambda *_: (0,) * len(shape))

    def send(start, size):
        width = size // UNITS
        block = slots * UNITS // STEPS
        grads = pl.BlockSpec((1, length, size), lambda m: (0, 0, start // size))
        return pl.pallas_call(
            functools.partial(send_kernel, **sizes),
            out_shape=jax.ShapeDtypeStruct((slots * UNITS, width), jnp.bfloat16),
            grid=(STEPS,),
            in_specs=[
                whole(1, length),
                whole(1, length),
                smem,
                smem,
                whole(1, length),
                whole(1, length),
                smem,
                grads,
                grads,
            ],
            out_specs=pl.BlockSpec((block, width), lambda m: (m, 0)),
            scratch_shapes=[
                pltpu.VMEM((1, 2 * length), jnp.int32),
                pltpu.VMEM((2 * length, size), jnp.bfloat16),
                pltpu.VMEM((width // 128, block, 128), jnp.float32),
            ],
            name="send",
        )(
            chosen_ids,
            rejected_ids,
            chosen_len,
            rejected_len,
            chosen_logp,
            rejected_logp,
            ref_logp,
            chosen_grads,
            rejected_grads,
        )

    def exchange(array):
        return lax.all_to_all(array, axes, split_axis=0, concat_axis=0, tiled=True)

    def receive(start, size, labels, arrived, table):
        width = size // UNITS
        block = slots * UNITS // STEPS
        operands = [labels, arrived]
        specs = [
            pl.BlockSpec((1, slots // STEPS), lambda k: (0, k)),
            pl.BlockSpec((block, width), lambda k: (k, 0)),
        ]
        aliases = {}
        if table is not None:
            operands.append(table)
            specs.append(pl.BlockSpec(memory_space=pl.ANY))
            aliases = {2: 0}
        return pl.pallas_call(
            receive_kernel,
            out_shape=jax.ShapeDtypeStruct((row_count, features), jnp.bfloat16),
            grid=(STEPS,),
            in_specs=specs,
            out_specs=pl.BlockSpec((row_count, size), lambda k: (0, start // size)),
            scratch_shapes=[
                pltpu.VMEM((padded, size), jnp.float32),
                pltpu.VMEM((width // 128, block, 128), jnp.float32),
            ],
            input_output_aliases=aliases,
            name="receive",
        )(*operands)

    starts = [sum(WIDTHS[:i]) for i in range(len(WIDTHS))]
    arrived = []
    for start, size in zip(starts, WIDTHS):
        sent = send(start, size).reshape(owners, capacity * UNITS, size // UNITS)
        arrived.append(exchange(sent).reshape(slots * UNITS, size // UNITS))
    labels = pl.pallas_call(
        functools.partial(label_kernel, **sizes),
        out_shape=jax.ShapeDtypeStruct((slots, 1), jnp.int32),
        name="label",
    )(chosen_ids, rejected_ids)
    labels = exchange(labels.reshape(owners, capacity)).reshape(1, slots)
    table = None
    for start, size, rows in zip(starts, WIDTHS, arrived):
        table = receive(start, size, labels, rows, table)
    return table


def solution(mesh):
    return jax.shard_map(
        local,
        mesh=mesh,
        in_specs=(
            P(("grp", "dp"), None),
            P(("grp", "dp"), None),
            P(("grp", "dp")),
            P(("grp", "dp")),
            P(("grp", "dp"), None),
            P(("grp", "dp"), None),
            P(None, ("grp", "dp")),
            P(("grp", "dp"), None, None),
            P(("grp", "dp"), None, None),
        ),
        out_specs=P(("grp", "dp"), None),
        check_vma=False,
    )
```

```python
import functools

import jax
import jax.numpy as jnp
from jax import lax
from jax.experimental import pallas as pl
from jax.experimental.pallas import tpu as pltpu
from jax.sharding import PartitionSpec as P


VOCAB = 128256
BETA = 0.1
XS, CORES, YS, ZS = 4, 2, 4, 8
PLANE = XS * CORES * YS
CAP = 6
DIRECT = 4
REST = CAP - DIRECT
LIMIT = 32
UNITS = 4
NOTE = 128
FLAG, ROUTE = 12, 13
STEP = 512

bf16 = jnp.bfloat16
f32 = jnp.float32
i32 = jnp.int32


def iota(shape, dim):
    return lax.broadcasted_iota(i32, shape, dim)


def onehot(hit):
    return jnp.where(hit, 1.0, 0.0).astype(bf16)


def dot(a, b):
    return jnp.dot(a, b, preferred_element_type=f32)


def dot_t(a, b):
    return lax.dot_general(a, b, (((1,), (1,)), ((), ())), preferred_element_type=f32)


def before(hits):
    tokens = hits.shape[1]
    block = 256
    earlier = onehot(iota((block, block), 0) < iota((block, block), 1))
    carry = jnp.zeros((hits.shape[0], 1), f32)
    counts = []
    for b in range(0, tokens, block):
        piece = hits[:, b : b + block]
        counts.append(dot(piece.astype(bf16), earlier) + carry)
        carry = carry + jnp.sum(piece, axis=1, keepdims=True)
    return jnp.concatenate(counts, axis=1)


def here():
    grp = lax.axis_index("grp")
    dp = lax.axis_index("dp")
    return dp & (ZS - 1), grp // CORES, grp & (CORES - 1), dp // ZS


def route(cid, rid, plan, note, row_count):
    ids = jnp.concatenate([cid[...], rid[...]], axis=1)
    owner = jnp.floor((ids.astype(f32) + 0.5) * (1.0 / row_count)).astype(i32)
    row = ids - owner * row_count
    mate = owner // ZS
    shift = (owner - here()[0]) & (ZS - 1)
    tokens = ids.shape[1]
    owners = PLANE * ZS
    near = jnp.where(iota((owners, tokens), 0) == shift * PLANE + mate, 1.0, 0.0)
    rank = jnp.sum(near * before(near), axis=0, keepdims=True).astype(i32)
    rest = rank >= DIRECT
    by_shift = jnp.where((iota((ZS, tokens), 0) == shift) & rest, 1.0, 0.0)
    order = jnp.sum(by_shift * before(by_shift), axis=0, keepdims=True).astype(i32)
    late = rest & (order >= LIMIT)
    first = jnp.where(rest & (order < LIMIT), shift * LIMIT + order, -1)
    plan[0:1] = jnp.where(rest, -1, owner * DIRECT + rank)
    plan[1:2] = first
    plan[2:3] = jnp.where(late, owner * REST + rank - DIRECT, -1)
    plan[3:8] = jnp.zeros((5, tokens), i32)
    over = jnp.max(jnp.where(late, 1.0, 0.0), axis=1, keepdims=True)
    lane = iota((NOTE, tokens), 0)
    code = jnp.where(lane == 2 * rank, row >> 4, 0) + jnp.where(lane == 2 * rank + 1, row & 15, 0)
    labels = dot_t(near.astype(bf16), code.astype(f32).astype(bf16))
    way = jnp.where(lane == ROUTE, mate * REST + (rank - DIRECT) + 1, 0)
    moved = onehot(iota((ZS * LIMIT, tokens), 0) == first)
    ways = dot_t(moved, way.astype(f32).astype(bf16))
    flag = jnp.where(iota((owners, NOTE), 1) == FLAG, over, 0.0)
    note[...] = (labels + ways + flag).astype(bf16)


def pair_weight(clen, rlen, clogp, rlogp, ref):
    length = clogp.shape[1]
    positions = iota((1, length), 1)
    chosen_mask = (positions >= length - clen[0]).astype(f32)
    rejected_mask = (positions >= length - rlen[0]).astype(f32)
    chosen = jnp.sum(chosen_mask * clogp[...], axis=1, keepdims=True)
    rejected = jnp.sum(rejected_mask * rlogp[...], axis=1, keepdims=True)
    margin = BETA * ((chosen - ref[0]) - (rejected - ref[1]))
    return BETA * (1.0 / (1.0 + jnp.exp(margin)))


def weighted(weight, cg, rg, rows):
    half = cg.shape[1]
    rows[:half] = (-weight[0:1, 0:1] * cg[0].astype(f32)).astype(bf16)
    rows[half:] = (weight[0:1, 0:1] * rg[0].astype(f32)).astype(bf16)


def first_kernel(cid, rid, clen, rlen, clogp, rlogp, ref, cg, rg, *refs, row_count):
    outs = refs[:ZS]
    plan, weight, note, pick = refs[ZS:]
    step = pl.program_id(0)
    last = pl.num_programs(0) - 1

    @pl.when(step == 0)
    def _():
        route(cid, rid, plan, note, row_count)
        weight[...] = jnp.broadcast_to(
            pair_weight(clen, rlen, clogp, rlogp, ref), weight.shape
        )
        pick[...] = onehot(iota(pick.shape, 0) == plan[1:2])

    @pl.when(step < last)
    def _():
        half = cg.shape[1]
        scale = weight[0:1, 0:1]
        moved = dot(pick[:, :half], cg[0]) * -scale + dot(pick[:, half:], rg[0]) * scale
        moved = moved.astype(bf16)
        for d in range(ZS):
            outs[d][...] = moved[d * LIMIT : d * LIMIT + LIMIT]

    @pl.when(step == last)
    def _():
        for d in range(ZS):
            outs[d][:, :NOTE] = note[d * LIMIT : d * LIMIT + LIMIT]


def direct_kernel(plan, weight, cg, rg, out, rows, pick, wide, *, kind):
    step = pl.program_id(0)

    @pl.when(step == 0)
    def _():
        pick[...] = onehot(iota(pick.shape, 0) == plan[kind : kind + 1])

    weighted(weight, cg, rg, rows)
    width = out.shape[1]
    slots = pick.shape[0]
    moved = dot(pick[...], rows[...])
    for u in range(UNITS):
        wide[pl.ds(u, slots, stride=UNITS), :] = moved[:, u * width : (u + 1) * width]
    out[...] = wide[...].astype(bf16)


def turned(index, place):
    y = (index + place[3]) & (YS - 1)
    core = (index // YS + place[2]) & (CORES - 1)
    x = (index // (YS * CORES) + place[1]) & (XS - 1)
    return (x * CORES + core) * YS + y


def second_kernel(*refs):
    place = here()
    arrived = refs[:ZS]
    notes = refs[ZS : 2 * ZS]
    outs = refs[2 * ZS : 2 * ZS + PLANE]
    pick, spread = refs[2 * ZS + PLANE :]
    step = pl.program_id(0)
    last = pl.num_programs(0) - 1
    each = ZS * REST

    @pl.when(step == 0)
    def _():
        note = jnp.concatenate([n[...] for n in notes], axis=0).astype(f32)
        blocks = [jnp.transpose(note[b : b + 128]) for b in range(0, ZS * LIMIT, 128)]
        route = jnp.concatenate(blocks, axis=1)[ROUTE : ROUTE + 1].astype(i32)
        out_row = iota(pick.shape, 0)
        in_row = iota(pick.shape, 1)
        mate = turned(out_row // each, place)
        shift = (out_row // REST) & (ZS - 1)
        wanted = mate * REST + (out_row & (REST - 1)) + 1
        pick[...] = onehot((in_row // LIMIT == shift) & (route == wanted))
        spread[...] = onehot(in_row == shift * PLANE + mate)

    @pl.when(step < last)
    def _():
        rows = jnp.concatenate([a[...] for a in arrived], axis=0)
        moved = dot(pick[...], rows).astype(bf16)
        for e in range(PLANE):
            outs[e][...] = moved[e * each : e * each + each]

    @pl.when(step == last)
    def _():
        note = jnp.concatenate([n[...] for n in notes], axis=0)
        moved = dot(spread[...], note).astype(bf16)
        for e in range(PLANE):
            outs[e][:, :NOTE] = moved[e * each : e * each + each]


def label_kernel(*refs):
    place = here()
    notes = refs[:PLANE]
    near, far, late, flag = refs[PLANE:]
    each = ZS * REST
    count = PLANE * each
    owners = PLANE * ZS
    note = jnp.concatenate([n[...] for n in notes], axis=0)
    wide = note.astype(f32)
    across = jnp.concatenate(
        [jnp.transpose(wide[b : b + 128]) for b in range(0, count, 128)], axis=1
    )
    flag[0] = jnp.max(across[FLAG : FLAG + 1]).astype(i32)

    def joined(across, ranks):
        which = iota((1, across.shape[1]), 1) % len(ranks)
        found = jnp.zeros(which.shape, f32)
        for i, rank in enumerate(ranks):
            high = across[2 * rank : 2 * rank + 1]
            low = across[2 * rank + 1 : 2 * rank + 2]
            found = found + jnp.where(which == i, 16.0 * high + low, 0.0)
        return found.astype(i32)

    straight = range(DIRECT)
    others = range(DIRECT, CAP)
    far[...] = joined(across, others)
    source = iota((owners, count), 0)
    item = iota((owners, count), 1)
    turn = item // each
    y = (place[3] - turn) & (YS - 1)
    core = (place[2] - turn // YS) & (CORES - 1)
    x = (place[1] - turn // (YS * CORES)) & (XS - 1)
    z = (place[0] - item // REST) & (ZS - 1)
    match = (source == ((x * CORES + core) * YS + y) * ZS + z) & ((item & (REST - 1)) == 0)
    by_source = dot(onehot(match), note).astype(bf16)
    for out, ranks in ((near, straight), (late, others)):
        places = owners * len(ranks)
        grow = onehot(iota((owners, places), 1) // len(ranks) == iota((owners, places), 0))
        grown = lax.dot_general(
            by_source, grow, (((0,), (0,)), ((), ())), preferred_element_type=f32
        )
        out[...] = joined(grown, ranks)


def finish_kernel(*refs, tiled):
    labels = refs[: tiled + 1]
    packed = refs[tiled + 1 : 2 * tiled + 1]
    parts = refs[2 * tiled + 1 : -4]
    out, wide, pick, rows = refs[-4:]
    step = pl.program_id(0)

    @pl.when(step == 0)
    def _():
        start = 0
        for label in labels:
            size = label.shape[1]
            block = pick.at[:, start : start + size]
            block[...] = onehot(iota(block.shape, 0) == label[...])
            start += size

    start = 0
    for block in packed:
        width = block.shape[1]
        slots = block.shape[0] // UNITS
        wide[: block.shape[0]] = block[...].astype(f32)
        for u in range(UNITS):
            rows[start : start + slots, u * width : (u + 1) * width] = wide[
                pl.ds(u, slots, stride=UNITS), :
            ].astype(bf16)
        start += slots
    for part in parts:
        rows[start : start + part.shape[0]] = part[...]
        start += part.shape[0]
    out[...] = dot(pick[...], rows[...])[: out.shape[0]].astype(bf16)


def shifted(dx, dcore, dy, dz):
    def at(x, core, y, z):
        return ((x % XS * CORES + core % CORES) * YS + y % YS) * ZS + z % ZS

    return [
        (at(x, core, y, z), at(x + dx, core + dcore, y + dy, z + dz))
        for x in range(XS)
        for core in range(CORES)
        for y in range(YS)
        for z in range(ZS)
    ]


def whole(*shape):
    return pl.BlockSpec(shape, lambda *_: (0,) * len(shape))


def local(cid, rid, clen, rlen, clogp, rlogp, ref, cg, rg):
    length, features = cg.shape[1:]
    tokens = 2 * length
    owners = PLANE * ZS
    row_count = VOCAB // owners
    axes = ("grp", "dp")
    smem = pl.BlockSpec(memory_space=pltpu.SMEM)
    columns = features + NOTE
    steps = features // STEP
    width = STEP // UNITS
    each = ZS * REST
    padded = (row_count + 15) // 16 * 16

    part = pl.BlockSpec((1, length, STEP), lambda n: (0, 0, jnp.minimum(n, steps - 1)))
    *first, plan, weight = pl.pallas_call(
        functools.partial(first_kernel, row_count=row_count),
        out_shape=[jax.ShapeDtypeStruct((LIMIT, columns), bf16)] * ZS
        + [jax.ShapeDtypeStruct((8, tokens), i32), jax.ShapeDtypeStruct((8, 128), f32)],
        grid=(steps + 1,),
        in_specs=[whole(1, length)] * 2
        + [smem] * 2
        + [whole(1, length)] * 2
        + [smem, part, part],
        out_specs=[pl.BlockSpec((LIMIT, STEP), lambda n: (0, n))] * ZS
        + [whole(8, tokens), whole(8, 128)],
        scratch_shapes=[
            pltpu.VMEM((owners, NOTE), bf16),
            pltpu.VMEM((ZS * LIMIT, tokens), bf16),
        ],
        name="first",
    )(cid, rid, clen, rlen, clogp, rlogp, ref.reshape(2), cg, rg)
    hopped = [first[0]] + [
        lax.ppermute(first[d], axes, shifted(0, 0, 0, d)) for d in range(1, ZS)
    ]

    def direct(kind, count):
        slots = owners * count
        sent = pl.pallas_call(
            functools.partial(direct_kernel, kind=kind),
            out_shape=jax.ShapeDtypeStruct((slots * UNITS, features // UNITS), bf16),
            grid=(steps,),
            in_specs=[
                whole(8, tokens),
                whole(8, 128),
                pl.BlockSpec((1, length, STEP), lambda n: (0, 0, n)),
                pl.BlockSpec((1, length, STEP), lambda n: (0, 0, n)),
            ],
            out_specs=pl.BlockSpec((slots * UNITS, width), lambda n: (0, n)),
            scratch_shapes=[
                pltpu.VMEM((tokens, STEP), bf16),
                pltpu.VMEM((slots, tokens), bf16),
                pltpu.VMEM((slots * UNITS, width), f32),
            ],
            name="direct",
        )(plan, weight, cg, rg)
        sent = sent.reshape(owners, count * UNITS, features // UNITS)
        sent = lax.all_to_all(sent, axes, split_axis=0, concat_axis=0, tiled=True)
        return sent.reshape(slots * UNITS, features // UNITS)

    arrived = direct(0, DIRECT)

    second = pl.pallas_call(
        second_kernel,
        out_shape=[jax.ShapeDtypeStruct((each, columns), bf16)] * PLANE,
        grid=(steps + 1,),
        in_specs=[pl.BlockSpec((LIMIT, STEP), lambda n: (0, jnp.minimum(n, steps - 1)))] * ZS
        + [pl.BlockSpec((LIMIT, NOTE), lambda n: (0, features // NOTE))] * ZS,
        out_specs=[pl.BlockSpec((each, STEP), lambda n: (0, n))] * PLANE,
        scratch_shapes=[
            pltpu.VMEM((PLANE * each, ZS * LIMIT), bf16),
            pltpu.VMEM((PLANE * each, ZS * LIMIT), bf16),
        ],
        name="second",
    )(*hopped, *hopped)
    turned_in = [second[0]]
    for e in range(1, PLANE):
        turn = (e // (YS * CORES), e // YS % CORES, e % YS)
        turned_in.append(lax.ppermute(second[e], axes, shifted(*turn, 0)))

    near, far, late, flag = pl.pallas_call(
        label_kernel,
        out_shape=[
            jax.ShapeDtypeStruct((1, owners * DIRECT), i32),
            jax.ShapeDtypeStruct((1, PLANE * each), i32),
            jax.ShapeDtypeStruct((1, owners * REST), i32),
            jax.ShapeDtypeStruct((1,), i32),
        ],
        grid=(1,),
        in_specs=[pl.BlockSpec((each, NOTE), lambda n: (0, features // NOTE))] * PLANE,
        out_specs=[
            whole(1, owners * DIRECT),
            whole(1, PLANE * each),
            whole(1, owners * REST),
            smem,
        ],
        name="label",
    )(*turned_in)

    def finish(labels, packed):
        count = sum(label.shape[1] for label in labels)
        tall = max(block.shape[0] for block in packed)
        return pl.pallas_call(
            functools.partial(finish_kernel, tiled=len(packed)),
            out_shape=jax.ShapeDtypeStruct((row_count, features), bf16),
            grid=(steps,),
            in_specs=[whole(*label.shape) for label in labels]
            + [pl.BlockSpec((block.shape[0], width), lambda n: (0, n)) for block in packed]
            + [pl.BlockSpec((each, STEP), lambda n: (0, n))] * PLANE,
            out_specs=pl.BlockSpec((row_count, STEP), lambda n: (0, n)),
            scratch_shapes=[
                pltpu.VMEM((tall, width), f32),
                pltpu.VMEM((padded, count), bf16),
                pltpu.VMEM((count, STEP), bf16),
            ],
            name="finish",
        )(*labels, *packed, *turned_in)

    return lax.cond(
        flag[0] > 0,
        lambda: finish([near, late, far], [arrived, direct(2, REST)]),
        lambda: finish([near, far], [arrived]),
    )


def solution(mesh):
    return jax.shard_map(
        local,
        mesh=mesh,
        in_specs=(
            P(("grp", "dp"), None),
            P(("grp", "dp"), None),
            P(("grp", "dp")),
            P(("grp", "dp")),
            P(("grp", "dp"), None),
            P(("grp", "dp"), None),
            P(None, ("grp", "dp")),
            P(("grp", "dp"), None, None),
            P(("grp", "dp"), None, None),
        ),
        out_specs=P(("grp", "dp"), None),
        check_vma=False,
    )
```

```python
import functools

import jax
import jax.numpy as jnp
from jax import lax
from jax.experimental import pallas as pl
from jax.experimental.pallas import tpu as pltpu
from jax.sharding import PartitionSpec as P


VOCAB = 128256
BETA = 0.1
XS, CORES, YS, ZS = 4, 2, 4, 8
PLANE = XS * CORES * YS
CAP = 6
DIRECT = 4
REST = CAP - DIRECT
LIMIT = 32
UNITS = 4
NOTE = 128
FLAG, ROUTE = 12, 13
STEP = 512
WIDE = 1024
CHUNK = 512
TURNS = XS * YS

bf16 = jnp.bfloat16
f32 = jnp.float32
i32 = jnp.int32


def iota(shape, dim):
    return lax.broadcasted_iota(i32, shape, dim)


def onehot(hit):
    return jnp.where(hit, 1.0, 0.0).astype(bf16)


def dot(a, b):
    return jnp.dot(a, b, preferred_element_type=f32)


def dot_t(a, b):
    return lax.dot_general(a, b, (((1,), (1,)), ((), ())), preferred_element_type=f32)


def before(hits):
    tokens = hits.shape[1]
    block = 256
    earlier = onehot(iota((block, block), 0) < iota((block, block), 1))
    carry = jnp.zeros((hits.shape[0], 1), f32)
    counts = []
    for b in range(0, tokens, block):
        piece = hits[:, b : b + block]
        counts.append(dot(piece.astype(bf16), earlier) + carry)
        carry = carry + jnp.sum(piece, axis=1, keepdims=True)
    return jnp.concatenate(counts, axis=1)


def here():
    grp = lax.axis_index("grp")
    dp = lax.axis_index("dp")
    return dp & (ZS - 1), grp // CORES, grp & (CORES - 1), dp // ZS


def route(cid, rid, plan, note, row_count):
    ids = jnp.concatenate([cid[...], rid[...]], axis=1)
    owner = jnp.floor((ids.astype(f32) + 0.5) * (1.0 / row_count)).astype(i32)
    row = ids - owner * row_count
    mate = owner // ZS
    shift = (owner - here()[0]) & (ZS - 1)
    tokens = ids.shape[1]
    owners = PLANE * ZS
    near = jnp.where(iota((owners, tokens), 0) == shift * PLANE + mate, 1.0, 0.0)
    rank = jnp.sum(near * before(near), axis=0, keepdims=True).astype(i32)
    rest = rank >= DIRECT
    by_shift = jnp.where((iota((ZS, tokens), 0) == shift) & rest, 1.0, 0.0)
    order = jnp.sum(by_shift * before(by_shift), axis=0, keepdims=True).astype(i32)
    late = rest & (order >= LIMIT)
    first = jnp.where(rest & (order < LIMIT), shift * LIMIT + order, -1)
    plan[0:1] = jnp.where(rest, -1, owner * DIRECT + rank)
    plan[1:2] = first
    plan[2:3] = jnp.where(late, owner * REST + rank - DIRECT, -1)
    plan[3:8] = jnp.zeros((5, tokens), i32)
    over = jnp.max(jnp.where(late, 1.0, 0.0), axis=1, keepdims=True)
    lane = iota((NOTE, tokens), 0)
    code = jnp.where(lane == 2 * rank, row >> 4, 0) + jnp.where(lane == 2 * rank + 1, row & 15, 0)
    labels = dot_t(near.astype(bf16), code.astype(f32).astype(bf16))
    way = jnp.where(lane == ROUTE, mate * REST + (rank - DIRECT) + 1, 0)
    moved = onehot(iota((ZS * LIMIT, tokens), 0) == first)
    ways = dot_t(moved, way.astype(f32).astype(bf16))
    flag = jnp.where(iota((owners, NOTE), 1) == FLAG, over, 0.0)
    note[...] = (labels + ways + flag).astype(bf16)


def pair_weight(clen, rlen, clogp, rlogp, ref):
    length = clogp.shape[1]
    positions = iota((1, length), 1)
    chosen_mask = (positions >= length - clen[0]).astype(f32)
    rejected_mask = (positions >= length - rlen[0]).astype(f32)
    chosen = jnp.sum(chosen_mask * clogp[...], axis=1, keepdims=True)
    rejected = jnp.sum(rejected_mask * rlogp[...], axis=1, keepdims=True)
    margin = BETA * ((chosen - ref[0]) - (rejected - ref[1]))
    return BETA * (1.0 / (1.0 + jnp.exp(margin)))


def weighted(weight, cg, rg, rows):
    half = cg.shape[1]
    rows[:half] = (-weight[0:1, 0:1] * cg[0].astype(f32)).astype(bf16)
    rows[half:] = (weight[0:1, 0:1] * rg[0].astype(f32)).astype(bf16)


def first_kernel(cid, rid, clen, rlen, clogp, rlogp, ref, cg, rg, *refs, row_count):
    outs = refs[:ZS]
    plan, weight, note, pick = refs[ZS:]
    step = pl.program_id(0)
    last = pl.num_programs(0) - 1

    @pl.when(step == 0)
    def _():
        route(cid, rid, plan, note, row_count)
        weight[...] = jnp.broadcast_to(
            pair_weight(clen, rlen, clogp, rlogp, ref), weight.shape
        )
        pick[...] = onehot(iota(pick.shape, 0) == plan[1:2])

    @pl.when(step < last)
    def _():
        half = cg.shape[1]
        scale = weight[0:1, 0:1]
        moved = dot(pick[:, :half], cg[0]) * -scale + dot(pick[:, half:], rg[0]) * scale
        moved = moved.astype(bf16)
        for d in range(ZS):
            outs[d][...] = moved[d * LIMIT : d * LIMIT + LIMIT]

    @pl.when(step == last)
    def _():
        for d in range(ZS):
            outs[d][:, :NOTE] = note[d * LIMIT : d * LIMIT + LIMIT]


def direct_kernel(plan, weight, cg, rg, out, rows, pick, wide, *, kind):
    step = pl.program_id(0)

    @pl.when(step == 0)
    def _():
        pick[...] = onehot(iota(pick.shape, 0) == plan[kind : kind + 1])

    weighted(weight, cg, rg, rows)
    width = out.shape[1]
    slots = pick.shape[0]
    moved = dot(pick[...], rows[...])
    for u in range(UNITS):
        wide[pl.ds(u, slots, stride=UNITS), :] = moved[:, u * width : (u + 1) * width]
    out[...] = wide[...].astype(bf16)


def turned(turn, swap, place):
    y = (turn + place[3]) & (YS - 1)
    core = (swap + place[2]) & (CORES - 1)
    x = (turn // YS + place[1]) & (XS - 1)
    return (x * CORES + core) * YS + y


def second_kernel(*refs):
    place = here()
    arrived = refs[:ZS]
    notes = refs[ZS : 2 * ZS]
    outs = refs[2 * ZS : 2 * ZS + TURNS]
    pick, spread = refs[2 * ZS + TURNS :]
    step = pl.program_id(0)
    last = pl.num_programs(0) - 1
    each = ZS * REST
    both = CORES * each

    @pl.when(step == 0)
    def _():
        note = jnp.concatenate([n[...] for n in notes], axis=0).astype(f32)
        blocks = [jnp.transpose(note[b : b + 128]) for b in range(0, ZS * LIMIT, 128)]
        way = jnp.concatenate(blocks, axis=1)[ROUTE : ROUTE + 1].astype(i32)
        out_row = iota(pick.shape, 0)
        in_row = iota(pick.shape, 1)
        mate = turned(out_row // both, out_row // each, place)
        shift = (out_row // REST) & (ZS - 1)
        wanted = mate * REST + (out_row & (REST - 1)) + 1
        pick[...] = onehot((in_row // LIMIT == shift) & (way == wanted))
        spread[...] = onehot(in_row == shift * PLANE + mate)

    @pl.when(step < last)
    def _():
        rows = jnp.concatenate([a[...] for a in arrived], axis=0)
        moved = dot(pick[...], rows).astype(bf16)
        for e in range(TURNS):
            outs[e][...] = moved[e * both : e * both + both]

    @pl.when(step == last)
    def _():
        note = jnp.concatenate([n[...] for n in notes], axis=0)
        moved = dot(spread[...], note).astype(bf16)
        for e in range(TURNS):
            outs[e][:, :NOTE] = moved[e * both : e * both + both]


def stack_kernel(*refs):
    out = refs[-1]
    for i, part in enumerate(refs[:-1]):
        out[i * part.shape[0] : (i + 1) * part.shape[0]] = part[...]


def collect_kernel(*refs):
    place = here()
    parts = refs[: TURNS + 1]
    notes = refs[TURNS + 1 : 2 * TURNS + 2]
    rows, near, far, late, flag = refs[2 * TURNS + 2 :]
    each = ZS * REST
    count = PLANE * each
    owners = PLANE * ZS
    start = 0
    for part in parts:
        rows[start : start + part.shape[0]] = part[...]
        start += part.shape[0]

    @pl.when(pl.program_id(0) == 0)
    def _():
        note = jnp.concatenate([n[...] for n in notes], axis=0)
        wide = note.astype(f32)
        across = jnp.concatenate(
            [jnp.transpose(wide[b : b + 128]) for b in range(0, count, 128)], axis=1
        )
        flag[0] = jnp.max(across[FLAG : FLAG + 1]).astype(i32)

        def joined(across, ranks):
            which = iota((1, across.shape[1]), 1) % len(ranks)
            found = jnp.zeros(which.shape, f32)
            for i, rank in enumerate(ranks):
                high = across[2 * rank : 2 * rank + 1]
                low = across[2 * rank + 1 : 2 * rank + 2]
                found = found + jnp.where(which == i, 16.0 * high + low, 0.0)
            return found.astype(i32)

        straight = range(DIRECT)
        others = range(DIRECT, CAP)
        far[...] = joined(across, others)
        source = iota((owners, count), 0)
        item = iota((owners, count), 1)
        turn = item // each
        y = (place[3] - turn) & (YS - 1)
        x = (place[1] - turn // YS) & (XS - 1)
        core = (place[2] - turn // TURNS) & (CORES - 1)
        z = (place[0] - item // REST) & (ZS - 1)
        match = (source == ((x * CORES + core) * YS + y) * ZS + z) & ((item & (REST - 1)) == 0)
        by_source = dot(onehot(match), note).astype(bf16)
        for out, ranks in ((near, straight), (late, others)):
            places = owners * len(ranks)
            grow = onehot(iota((owners, places), 1) // len(ranks) == iota((owners, places), 0))
            grown = lax.dot_general(
                by_source, grow, (((0,), (0,)), ((), ())), preferred_element_type=f32
            )
            out[...] = joined(grown, ranks)


def finish_kernel(*refs, tiled):
    labels = refs[: tiled + 1]
    packed = refs[tiled + 1 : 2 * tiled + 1]
    rest = refs[2 * tiled + 1]
    out, pick, *scratch = refs[2 * tiled + 2 :]
    step = pl.program_id(0)
    half = CHUNK

    @pl.when(step == 0)
    def _():
        start = 0
        for label in labels:
            size = label.shape[1]
            block = pick.at[:, start : start + size]
            block[...] = onehot(iota(block.shape, 0) == label[...])
            start += size

    total = dot(pick[:, -rest.shape[0] :], rest[...])
    start = 0
    for block in packed:
        width = block.shape[1]
        for first in range(0, block.shape[0] // UNITS, half):
            wide, rows = scratch[2 * (start // half % 2) : 2 * (start // half % 2) + 2]
            wide[...] = block[first * UNITS : (first + half) * UNITS].astype(f32)
            for u in range(UNITS):
                rows[:, u * width : (u + 1) * width] = wide[
                    pl.ds(u, half, stride=UNITS), :
                ].astype(bf16)
            total += dot(pick[:, start : start + half], rows[...])
            start += half
    out[...] = total[: out.shape[0]].astype(bf16)


def shifted(dx, dcore, dy, dz):
    def at(x, core, y, z):
        return ((x % XS * CORES + core % CORES) * YS + y % YS) * ZS + z % ZS

    return [
        (at(x, core, y, z), at(x + dx, core + dcore, y + dy, z + dz))
        for x in range(XS)
        for core in range(CORES)
        for y in range(YS)
        for z in range(ZS)
    ]


def whole(*shape):
    return pl.BlockSpec(shape, lambda *_: (0,) * len(shape))


def local(cid, rid, clen, rlen, clogp, rlogp, ref, cg, rg):
    length, features = cg.shape[1:]
    tokens = 2 * length
    owners = PLANE * ZS
    row_count = VOCAB // owners
    axes = ("grp", "dp")
    smem = pl.BlockSpec(memory_space=pltpu.SMEM)
    columns = features + NOTE
    steps = features // STEP
    width = STEP // UNITS
    each = ZS * REST
    padded = (row_count + 15) // 16 * 16

    few = features // WIDE
    part = pl.BlockSpec((1, length, WIDE), lambda n: (0, 0, jnp.minimum(n, few - 1)))
    *first, plan, weight = pl.pallas_call(
        functools.partial(first_kernel, row_count=row_count),
        out_shape=[jax.ShapeDtypeStruct((LIMIT, columns), bf16)] * ZS
        + [jax.ShapeDtypeStruct((8, tokens), i32), jax.ShapeDtypeStruct((8, 128), f32)],
        grid=(few + 1,),
        in_specs=[whole(1, length)] * 2
        + [smem] * 2
        + [whole(1, length)] * 2
        + [smem, part, part],
        out_specs=[pl.BlockSpec((LIMIT, WIDE), lambda n: (0, n))] * ZS
        + [whole(8, tokens), whole(8, 128)],
        scratch_shapes=[
            pltpu.VMEM((owners, NOTE), bf16),
            pltpu.VMEM((ZS * LIMIT, tokens), bf16),
        ],
        name="first",
    )(cid, rid, clen, rlen, clogp, rlogp, ref.reshape(2), cg, rg)
    hopped = [first[0]] + [
        lax.ppermute(first[d], axes, shifted(0, 0, 0, d)) for d in range(1, ZS)
    ]

    def direct(kind, count):
        slots = owners * count
        sent = pl.pallas_call(
            functools.partial(direct_kernel, kind=kind),
            out_shape=jax.ShapeDtypeStruct((slots * UNITS, features // UNITS), bf16),
            grid=(steps,),
            in_specs=[
                whole(8, tokens),
                whole(8, 128),
                pl.BlockSpec((1, length, STEP), lambda n: (0, 0, n)),
                pl.BlockSpec((1, length, STEP), lambda n: (0, 0, n)),
            ],
            out_specs=pl.BlockSpec((slots * UNITS, width), lambda n: (0, n)),
            scratch_shapes=[
                pltpu.VMEM((tokens, STEP), bf16),
                pltpu.VMEM((slots, tokens), bf16),
                pltpu.VMEM((slots * UNITS, width), f32),
            ],
            name="direct",
        )(plan, weight, cg, rg)
        sent = sent.reshape(owners, count * UNITS, features // UNITS)
        sent = lax.all_to_all(sent, axes, split_axis=0, concat_axis=0, tiled=True)
        return sent.reshape(slots * UNITS, features // UNITS)

    arrived = direct(0, DIRECT)

    both = CORES * each
    here_part = [pl.BlockSpec((LIMIT, WIDE), lambda n: (0, jnp.minimum(n, few - 1)))] * ZS
    here_note = [pl.BlockSpec((LIMIT, NOTE), lambda n: (0, features // NOTE))] * ZS
    second = pl.pallas_call(
        second_kernel,
        out_shape=[jax.ShapeDtypeStruct((both, columns), bf16)] * TURNS,
        grid=(few + 1,),
        in_specs=here_part + here_note,
        out_specs=[pl.BlockSpec((both, WIDE), lambda n: (0, n))] * TURNS,
        scratch_shapes=[
            pltpu.VMEM((PLANE * each, ZS * LIMIT), bf16),
            pltpu.VMEM((PLANE * each, ZS * LIMIT), bf16),
        ],
        name="second",
    )(*hopped, *hopped)
    turns = [second[0]] + [
        lax.ppermute(second[e], axes, shifted(e // YS, 0, e % YS, 0)) for e in range(1, TURNS)
    ]
    swap = pl.pallas_call(
        stack_kernel,
        out_shape=jax.ShapeDtypeStruct((TURNS * each, columns), bf16),
        grid=(few + 1,),
        in_specs=[pl.BlockSpec((each, WIDE), lambda n: (1, n))] * TURNS,
        out_specs=pl.BlockSpec((TURNS * each, WIDE), lambda n: (0, n)),
        name="stack",
    )(*turns)
    swap = lax.ppermute(swap, axes, shifted(0, 1, 0, 0))

    rest, near, far, late, flag = pl.pallas_call(
        collect_kernel,
        out_shape=[
            jax.ShapeDtypeStruct((PLANE * each, features), bf16),
            jax.ShapeDtypeStruct((1, owners * DIRECT), i32),
            jax.ShapeDtypeStruct((1, PLANE * each), i32),
            jax.ShapeDtypeStruct((1, owners * REST), i32),
            jax.ShapeDtypeStruct((1,), i32),
        ],
        grid=(few,),
        in_specs=[pl.BlockSpec((each, WIDE), lambda n: (0, n))] * TURNS
        + [pl.BlockSpec((TURNS * each, WIDE), lambda n: (0, n))]
        + [pl.BlockSpec((each, NOTE), lambda n: (0, features // NOTE))] * TURNS
        + [pl.BlockSpec((TURNS * each, NOTE), lambda n: (0, features // NOTE))],
        out_specs=[
            pl.BlockSpec((PLANE * each, WIDE), lambda n: (0, n)),
            whole(1, owners * DIRECT),
            whole(1, PLANE * each),
            whole(1, owners * REST),
            smem,
        ],
        name="collect",
    )(*turns, swap, *turns, swap)

    def finish(labels, packed):
        count = sum(label.shape[1] for label in labels)
        return pl.pallas_call(
            functools.partial(finish_kernel, tiled=len(packed)),
            out_shape=jax.ShapeDtypeStruct((row_count, features), bf16),
            grid=(steps,),
            in_specs=[whole(*label.shape) for label in labels]
            + [pl.BlockSpec((block.shape[0], width), lambda n: (0, n)) for block in packed]
            + [pl.BlockSpec((PLANE * each, STEP), lambda n: (0, n))],
            out_specs=pl.BlockSpec((row_count, STEP), lambda n: (0, n)),
            scratch_shapes=[pltpu.VMEM((padded, count), bf16)]
            + [
                pltpu.VMEM((CHUNK * UNITS, width), f32),
                pltpu.VMEM((CHUNK, STEP), bf16),
            ]
            * 2,
            name="finish",
        )(*labels, *packed, rest)

    return lax.cond(
        flag[0] > 0,
        lambda: finish([near, late, far], [arrived, direct(2, REST)]),
        lambda: finish([near, far], [arrived]),
    )


def solution(mesh):
    return jax.shard_map(
        local,
        mesh=mesh,
        in_specs=(
            P(("grp", "dp"), None),
            P(("grp", "dp"), None),
            P(("grp", "dp")),
            P(("grp", "dp")),
            P(("grp", "dp"), None),
            P(("grp", "dp"), None),
            P(None, ("grp", "dp")),
            P(("grp", "dp"), None, None),
            P(("grp", "dp"), None, None),
        ),
        out_specs=P(("grp", "dp"), None),
        check_vma=False,
    )
```

```python
import functools

import jax
import jax.numpy as jnp
from jax import lax
from jax.experimental import pallas as pl
from jax.experimental.pallas import tpu as pltpu
from jax.sharding import PartitionSpec as P


VOCAB = 128256
BETA = 0.1
XS, CORES, YS, ZS = 4, 2, 4, 8
PLANE = XS * CORES * YS
CAP = 6
DIRECT = 4
REST = CAP - DIRECT
LIMIT = 32
UNITS = 4
NOTE = 128
FLAG, ROUTE = 12, 13
STEP = 512
WIDE = 1024
CHUNK = 512
TURNS = XS * YS

bf16 = jnp.bfloat16
f32 = jnp.float32
i32 = jnp.int32


def iota(shape, dim):
    return lax.broadcasted_iota(i32, shape, dim)


def onehot(hit):
    return jnp.where(hit, 1.0, 0.0).astype(bf16)


def dot(a, b):
    return jnp.dot(a, b, preferred_element_type=f32)


def dot_t(a, b):
    return lax.dot_general(a, b, (((1,), (1,)), ((), ())), preferred_element_type=f32)


def before(hits):
    tokens = hits.shape[1]
    block = 256
    earlier = onehot(iota((block, block), 0) < iota((block, block), 1))
    carry = jnp.zeros((hits.shape[0], 1), f32)
    counts = []
    for b in range(0, tokens, block):
        piece = hits[:, b : b + block]
        counts.append(dot(piece.astype(bf16), earlier) + carry)
        carry = carry + jnp.sum(piece, axis=1, keepdims=True)
    return jnp.concatenate(counts, axis=1)


def here():
    grp = lax.axis_index("grp")
    dp = lax.axis_index("dp")
    return dp & (ZS - 1), grp // CORES, grp & (CORES - 1), dp // ZS


def route(cid, rid, plan, note, row_count):
    ids = jnp.concatenate([cid[...], rid[...]], axis=1)
    owner = jnp.floor((ids.astype(f32) + 0.5) * (1.0 / row_count)).astype(i32)
    row = ids - owner * row_count
    mate = owner // ZS
    shift = (owner - here()[0]) & (ZS - 1)
    tokens = ids.shape[1]
    owners = PLANE * ZS
    near = jnp.where(iota((owners, tokens), 0) == shift * PLANE + mate, 1.0, 0.0)
    rank = jnp.sum(near * before(near), axis=0, keepdims=True).astype(i32)
    rest = rank >= DIRECT
    by_shift = jnp.where((iota((ZS, tokens), 0) == shift) & rest, 1.0, 0.0)
    order = jnp.sum(by_shift * before(by_shift), axis=0, keepdims=True).astype(i32)
    late = rest & (order >= LIMIT)
    first = jnp.where(rest & (order < LIMIT), shift * LIMIT + order, -1)
    plan[0:1] = jnp.where(rest, -1, owner * DIRECT + rank)
    plan[1:2] = first
    plan[2:3] = jnp.where(late, owner * REST + rank - DIRECT, -1)
    plan[3:8] = jnp.zeros((5, tokens), i32)
    over = jnp.max(jnp.where(late, 1.0, 0.0), axis=1, keepdims=True)
    lane = iota((NOTE, tokens), 0)
    code = jnp.where(lane == 2 * rank, row >> 4, 0) + jnp.where(lane == 2 * rank + 1, row & 15, 0)
    labels = dot_t(near.astype(bf16), code.astype(f32).astype(bf16))
    way = jnp.where(lane == ROUTE, mate * REST + (rank - DIRECT) + 1, 0)
    moved = onehot(iota((ZS * LIMIT, tokens), 0) == first)
    ways = dot_t(moved, way.astype(f32).astype(bf16))
    flag = jnp.where(iota((owners, NOTE), 1) == FLAG, over, 0.0)
    note[...] = (labels + ways + flag).astype(bf16)


def pair_weight(clen, rlen, clogp, rlogp, ref):
    length = clogp.shape[1]
    positions = iota((1, length), 1)
    chosen_mask = (positions >= length - clen[0]).astype(f32)
    rejected_mask = (positions >= length - rlen[0]).astype(f32)
    chosen = jnp.sum(chosen_mask * clogp[...], axis=1, keepdims=True)
    rejected = jnp.sum(rejected_mask * rlogp[...], axis=1, keepdims=True)
    margin = BETA * ((chosen - ref[0]) - (rejected - ref[1]))
    return BETA * (1.0 / (1.0 + jnp.exp(margin)))


def weighted(weight, cg, rg, rows):
    half = cg.shape[1]
    rows[:half] = (-weight[0:1, 0:1] * cg[0].astype(f32)).astype(bf16)
    rows[half:] = (weight[0:1, 0:1] * rg[0].astype(f32)).astype(bf16)


def first_kernel(cid, rid, clen, rlen, clogp, rlogp, ref, cg, rg, *refs, row_count):
    outs = refs[:ZS]
    plan, weight, note, pick, rows, arrival = refs[ZS:]
    step = pl.program_id(0)
    last = pl.num_programs(0) - 1
    half = cg.shape[1]
    few = rows.shape[0]

    def fetches(n):
        columns = pl.ds(n * WIDE, WIDE)
        return [
            pltpu.make_async_copy(
                grads.at[0, :, columns], rows.at[n, pl.ds(i * half, half)], arrival.at[n, i]
            )
            for i, grads in enumerate((cg, rg))
        ]

    @pl.when(step == 0)
    def _():
        for n in range(few):
            for fetch in fetches(n):
                fetch.start()
        route(cid, rid, plan, note, row_count)
        weight[...] = jnp.broadcast_to(
            pair_weight(clen, rlen, clogp, rlogp, ref), weight.shape
        )
        pick[...] = onehot(iota(pick.shape, 0) == plan[1:2])

    @pl.when(step < last)
    def _():
        for fetch in fetches(step):
            fetch.wait()
        scale = weight[0:1, 0:1]
        moved = dot(pick[:, :half], rows[step, :half]) * -scale
        moved += dot(pick[:, half:], rows[step, half:]) * scale
        moved = moved.astype(bf16)
        for d in range(ZS):
            outs[d][...] = moved[d * LIMIT : d * LIMIT + LIMIT]

    @pl.when(step == last)
    def _():
        for d in range(ZS):
            outs[d][:, :NOTE] = note[d * LIMIT : d * LIMIT + LIMIT]


def direct_kernel(plan, weight, cg, rg, out, rows, pick, wide, *, kind):
    step = pl.program_id(0)

    @pl.when(step == 0)
    def _():
        pick[...] = onehot(iota(pick.shape, 0) == plan[kind : kind + 1])

    weighted(weight, cg, rg, rows)
    width = out.shape[2]
    slots = pick.shape[0]
    moved = dot(pick[...], rows[...])
    for u in range(UNITS):
        wide[pl.ds(u, slots, stride=UNITS), :] = moved[:, u * width : (u + 1) * width]
    out[...] = wide[...].astype(bf16).reshape(out.shape)


def turned(turn, swap, place):
    y = (turn + place[3]) & (YS - 1)
    core = (swap + place[2]) & (CORES - 1)
    x = (turn // YS + place[1]) & (XS - 1)
    return (x * CORES + core) * YS + y


def second_kernel(*refs):
    place = here()
    arrived = refs[:ZS]
    notes = refs[ZS : 2 * ZS]
    outs = refs[2 * ZS : 2 * ZS + TURNS]
    pick, spread = refs[2 * ZS + TURNS :]
    step = pl.program_id(0)
    last = pl.num_programs(0) - 1
    each = ZS * REST
    both = CORES * each

    @pl.when(step == 0)
    def _():
        note = jnp.concatenate([n[...] for n in notes], axis=0).astype(f32)
        blocks = [jnp.transpose(note[b : b + 128]) for b in range(0, ZS * LIMIT, 128)]
        way = jnp.concatenate(blocks, axis=1)[ROUTE : ROUTE + 1].astype(i32)
        out_row = iota(pick.shape, 0)
        in_row = iota(pick.shape, 1)
        mate = turned(out_row // both, out_row // each, place)
        shift = (out_row // REST) & (ZS - 1)
        wanted = mate * REST + (out_row & (REST - 1)) + 1
        pick[...] = onehot((in_row // LIMIT == shift) & (way == wanted))
        spread[...] = onehot(in_row == shift * PLANE + mate)

    @pl.when(step < last)
    def _():
        rows = jnp.concatenate([a[...] for a in arrived], axis=0)
        moved = dot(pick[...], rows).astype(bf16)
        for e in range(TURNS):
            outs[e][...] = moved[e * both : e * both + both]

    @pl.when(step == last)
    def _():
        note = jnp.concatenate([n[...] for n in notes], axis=0)
        moved = dot(spread[...], note).astype(bf16)
        for e in range(TURNS):
            outs[e][:, :NOTE] = moved[e * both : e * both + both]


def stack_kernel(*refs):
    out = refs[-1]
    for i, part in enumerate(refs[:-1]):
        out[i * part.shape[0] : (i + 1) * part.shape[0]] = part[...]


def collect_kernel(*refs):
    place = here()
    parts = refs[: TURNS + 1]
    notes = refs[TURNS + 1 : 2 * TURNS + 2]
    rows, near, far, late, flag = refs[2 * TURNS + 2 :]
    each = ZS * REST
    count = PLANE * each
    owners = PLANE * ZS
    start = 0
    for part in parts:
        rows[start : start + part.shape[0]] = part[...]
        start += part.shape[0]

    @pl.when(pl.program_id(0) == 0)
    def _():
        note = jnp.concatenate([n[...] for n in notes], axis=0)
        wide = note.astype(f32)
        across = jnp.concatenate(
            [jnp.transpose(wide[b : b + 128]) for b in range(0, count, 128)], axis=1
        )
        flag[0] = jnp.max(across[FLAG : FLAG + 1]).astype(i32)

        def joined(across, ranks):
            which = iota((1, across.shape[1]), 1) % len(ranks)
            found = jnp.zeros(which.shape, f32)
            for i, rank in enumerate(ranks):
                high = across[2 * rank : 2 * rank + 1]
                low = across[2 * rank + 1 : 2 * rank + 2]
                found = found + jnp.where(which == i, 16.0 * high + low, 0.0)
            return found.astype(i32)

        straight = range(DIRECT)
        others = range(DIRECT, CAP)
        far[...] = joined(across, others)
        source = iota((owners, count), 0)
        item = iota((owners, count), 1)
        turn = item // each
        y = (place[3] - turn) & (YS - 1)
        x = (place[1] - turn // YS) & (XS - 1)
        core = (place[2] - turn // TURNS) & (CORES - 1)
        z = (place[0] - item // REST) & (ZS - 1)
        match = (source == ((x * CORES + core) * YS + y) * ZS + z) & ((item & (REST - 1)) == 0)
        by_source = dot(onehot(match), note).astype(bf16)
        for out, ranks in ((near, straight), (late, others)):
            places = owners * len(ranks)
            grow = onehot(iota((owners, places), 1) // len(ranks) == iota((owners, places), 0))
            grown = lax.dot_general(
                by_source, grow, (((0,), (0,)), ((), ())), preferred_element_type=f32
            )
            out[...] = joined(grown, ranks)


def finish_kernel(*refs, tiled):
    labels = refs[: tiled + 1]
    packed = refs[tiled + 1 : 2 * tiled + 1]
    rest = refs[2 * tiled + 1]
    out, pick, *scratch = refs[2 * tiled + 2 : 2 * tiled + 8]
    *blocks, others, arrival = refs[2 * tiled + 8 :]
    step = pl.program_id(0)

    def fetches(n):
        pairs = []
        for source, block in zip(packed, blocks):
            tall = block.shape[2]
            pairs.append((source.at[:, pl.ds(n * tall, tall)], block.at[n]))
        pairs.append((rest.at[:, pl.ds(n * STEP, STEP)], others.at[n]))
        return [
            pltpu.make_async_copy(source, target, arrival.at[n, i])
            for i, (source, target) in enumerate(pairs)
        ]

    @pl.when(step == 0)
    def _():
        for n in range(others.shape[0]):
            for fetch in fetches(n):
                fetch.start()
        start = 0
        for label in labels:
            size = label.shape[1]
            part = pick.at[:, start : start + size]
            part[...] = onehot(iota(part.shape, 0) == label[...])
            start += size

    for fetch in fetches(step):
        fetch.wait()
    total = dot(pick[:, -rest.shape[0] :], others[step])
    start = 0
    for block in blocks:
        _, count, tall, width = block.shape
        piece = CHUNK * UNITS // tall
        for first in range(0, count, piece):
            side = 2 * (start // CHUNK % 2)
            wide, rows = scratch[side : side + 2]
            wide[...] = block[step, first : first + piece].astype(f32).reshape(wide.shape)
            for u in range(UNITS):
                unit = wide[pl.ds(u, CHUNK, stride=UNITS), :].astype(bf16)
                rows[:, u * width : (u + 1) * width] = unit
            total += dot(pick[:, start : start + CHUNK], rows[...])
            start += CHUNK
    out[...] = total[: out.shape[0]].astype(bf16)


def shifted(dx, dcore, dy, dz):
    def at(x, core, y, z):
        return ((x % XS * CORES + core % CORES) * YS + y % YS) * ZS + z % ZS

    return [
        (at(x, core, y, z), at(x + dx, core + dcore, y + dy, z + dz))
        for x in range(XS)
        for core in range(CORES)
        for y in range(YS)
        for z in range(ZS)
    ]


def whole(*shape):
    return pl.BlockSpec(shape, lambda *_: (0,) * len(shape))


def local(cid, rid, clen, rlen, clogp, rlogp, ref, cg, rg):
    length, features = cg.shape[1:]
    tokens = 2 * length
    owners = PLANE * ZS
    row_count = VOCAB // owners
    axes = ("grp", "dp")
    smem = pl.BlockSpec(memory_space=pltpu.SMEM)
    columns = features + NOTE
    steps = features // STEP
    width = STEP // UNITS
    each = ZS * REST
    padded = (row_count + 15) // 16 * 16

    few = features // WIDE
    *first, plan, weight = pl.pallas_call(
        functools.partial(first_kernel, row_count=row_count),
        out_shape=[jax.ShapeDtypeStruct((LIMIT, columns), bf16)] * ZS
        + [jax.ShapeDtypeStruct((8, tokens), i32), jax.ShapeDtypeStruct((8, 128), f32)],
        grid=(few + 1,),
        in_specs=[whole(1, length)] * 2
        + [smem] * 2
        + [whole(1, length)] * 2
        + [smem] + [pl.BlockSpec(memory_space=pl.ANY)] * 2,
        out_specs=[pl.BlockSpec((LIMIT, WIDE), lambda n: (0, n))] * ZS
        + [whole(8, tokens), whole(8, 128)],
        scratch_shapes=[
            pltpu.VMEM((owners, NOTE), bf16),
            pltpu.VMEM((ZS * LIMIT, tokens), bf16),
            pltpu.VMEM((few, tokens, WIDE), bf16),
            pltpu.SemaphoreType.DMA((few, 2)),
        ],
        name="first",
    )(cid, rid, clen, rlen, clogp, rlogp, ref.reshape(2), cg, rg)
    hopped = [first[0]] + [
        lax.ppermute(first[d], axes, shifted(0, 0, 0, d)) for d in range(1, ZS)
    ]

    def direct(kind, count):
        slots = owners * count
        sent = pl.pallas_call(
            functools.partial(direct_kernel, kind=kind),
            out_shape=jax.ShapeDtypeStruct((owners, steps * count * UNITS, width), bf16),
            grid=(steps,),
            in_specs=[
                whole(8, tokens),
                whole(8, 128),
                pl.BlockSpec((1, length, STEP), lambda n: (0, 0, n)),
                pl.BlockSpec((1, length, STEP), lambda n: (0, 0, n)),
            ],
            out_specs=pl.BlockSpec((owners, count * UNITS, width), lambda n: (0, n, 0)),
            scratch_shapes=[
                pltpu.VMEM((tokens, STEP), bf16),
                pltpu.VMEM((slots, tokens), bf16),
                pltpu.VMEM((slots * UNITS, width), f32),
            ],
            name="direct",
        )(plan, weight, cg, rg)
        return lax.all_to_all(sent, axes, split_axis=0, concat_axis=0, tiled=True)

    arrived = direct(0, DIRECT)

    both = CORES * each
    here_part = [pl.BlockSpec((LIMIT, WIDE), lambda n: (0, jnp.minimum(n, few - 1)))] * ZS
    here_note = [pl.BlockSpec((LIMIT, NOTE), lambda n: (0, features // NOTE))] * ZS
    second = pl.pallas_call(
        second_kernel,
        out_shape=[jax.ShapeDtypeStruct((both, columns), bf16)] * TURNS,
        grid=(few + 1,),
        in_specs=here_part + here_note,
        out_specs=[pl.BlockSpec((both, WIDE), lambda n: (0, n))] * TURNS,
        scratch_shapes=[
            pltpu.VMEM((PLANE * each, ZS * LIMIT), bf16),
            pltpu.VMEM((PLANE * each, ZS * LIMIT), bf16),
        ],
        name="second",
    )(*hopped, *hopped)
    turns = [second[0]] + [
        lax.ppermute(second[e], axes, shifted(e // YS, 0, e % YS, 0)) for e in range(1, TURNS)
    ]
    swap = pl.pallas_call(
        stack_kernel,
        out_shape=jax.ShapeDtypeStruct((TURNS * each, columns), bf16),
        grid=(few + 1,),
        in_specs=[pl.BlockSpec((each, WIDE), lambda n: (1, n))] * TURNS,
        out_specs=pl.BlockSpec((TURNS * each, WIDE), lambda n: (0, n)),
        name="stack",
    )(*turns)
    swap = lax.ppermute(swap, axes, shifted(0, 1, 0, 0))

    rest, near, far, late, flag = pl.pallas_call(
        collect_kernel,
        out_shape=[
            jax.ShapeDtypeStruct((PLANE * each, features), bf16),
            jax.ShapeDtypeStruct((1, owners * DIRECT), i32),
            jax.ShapeDtypeStruct((1, PLANE * each), i32),
            jax.ShapeDtypeStruct((1, owners * REST), i32),
            jax.ShapeDtypeStruct((1,), i32),
        ],
        grid=(few,),
        in_specs=[pl.BlockSpec((each, WIDE), lambda n: (0, n))] * TURNS
        + [pl.BlockSpec((TURNS * each, WIDE), lambda n: (0, n))]
        + [pl.BlockSpec((each, NOTE), lambda n: (0, features // NOTE))] * TURNS
        + [pl.BlockSpec((TURNS * each, NOTE), lambda n: (0, features // NOTE))],
        out_specs=[
            pl.BlockSpec((PLANE * each, WIDE), lambda n: (0, n)),
            whole(1, owners * DIRECT),
            whole(1, PLANE * each),
            whole(1, owners * REST),
            smem,
        ],
        name="collect",
    )(*turns, swap, *turns, swap)

    def finish(labels, packed):
        count = sum(label.shape[1] for label in labels)
        return pl.pallas_call(
            functools.partial(finish_kernel, tiled=len(packed)),
            out_shape=jax.ShapeDtypeStruct((row_count, features), bf16),
            grid=(steps,),
            in_specs=[whole(*label.shape) for label in labels]
            + [pl.BlockSpec(memory_space=pl.ANY)] * (len(packed) + 1),
            out_specs=pl.BlockSpec((row_count, STEP), lambda n: (0, n)),
            scratch_shapes=[pltpu.VMEM((padded, count), bf16)]
            + [
                pltpu.VMEM((CHUNK * UNITS, width), f32),
                pltpu.VMEM((CHUNK, STEP), bf16),
            ]
            * 2
            + [
                pltpu.VMEM((steps, owners, block.shape[1] // steps, width), bf16)
                for block in packed
            ]
            + [
                pltpu.VMEM((steps, PLANE * each, STEP), bf16),
                pltpu.SemaphoreType.DMA((steps, len(packed) + 1)),
            ],
            name="finish",
        )(*labels, *packed, rest)

    return lax.cond(
        flag[0] > 0,
        lambda: finish([near, late, far], [arrived, direct(2, REST)]),
        lambda: finish([near, far], [arrived]),
    )


def solution(mesh):
    return jax.shard_map(
        local,
        mesh=mesh,
        in_specs=(
            P(("grp", "dp"), None),
            P(("grp", "dp"), None),
            P(("grp", "dp")),
            P(("grp", "dp")),
            P(("grp", "dp"), None),
            P(("grp", "dp"), None),
            P(None, ("grp", "dp")),
            P(("grp", "dp"), None, None),
            P(("grp", "dp"), None, None),
        ),
        out_specs=P(("grp", "dp"), None),
        check_vma=False,
    )
```

```python
import functools

import jax
import jax.numpy as jnp
from jax import lax
from jax.experimental import pallas as pl
from jax.experimental.pallas import tpu as pltpu
from jax.sharding import PartitionSpec as P


VOCAB = 128256
BETA = 0.1
XS, CORES, YS, ZS = 4, 2, 4, 8
PLANE = XS * CORES * YS
CAP = 6
DIRECT = 4
REST = CAP - DIRECT
LIMIT = 32
UNITS = 4
NOTE = 128
FLAG, ROUTE = 12, 13
STEP = 512
WIDE = 1024
CHUNK = 512
WAYS = sorted(range(1, ZS), key=lambda d: -min(d, ZS - d))
TURNS = XS * YS

bf16 = jnp.bfloat16
f32 = jnp.float32
i32 = jnp.int32


def iota(shape, dim):
    return lax.broadcasted_iota(i32, shape, dim)


def onehot(hit):
    return jnp.where(hit, 1.0, 0.0).astype(bf16)


def dot(a, b):
    return jnp.dot(a, b, preferred_element_type=f32)


def dot_t(a, b):
    return lax.dot_general(a, b, (((1,), (1,)), ((), ())), preferred_element_type=f32)


def before(hits):
    tokens = hits.shape[1]
    block = 256
    earlier = onehot(iota((block, block), 0) < iota((block, block), 1))
    carry = jnp.zeros((hits.shape[0], 1), f32)
    counts = []
    for b in range(0, tokens, block):
        piece = hits[:, b : b + block]
        counts.append(dot(piece.astype(bf16), earlier) + carry)
        carry = carry + jnp.sum(piece, axis=1, keepdims=True)
    return jnp.concatenate(counts, axis=1)


def here():
    grp = lax.axis_index("grp")
    dp = lax.axis_index("dp")
    return dp & (ZS - 1), grp // CORES, grp & (CORES - 1), dp // ZS


def route(cid, rid, plan, note, row_count):
    ids = jnp.concatenate([cid[...], rid[...]], axis=1)
    owner = jnp.floor((ids.astype(f32) + 0.5) * (1.0 / row_count)).astype(i32)
    row = ids - owner * row_count
    mate = owner // ZS
    shift = (owner - here()[0]) & (ZS - 1)
    tokens = ids.shape[1]
    owners = PLANE * ZS
    near = jnp.where(iota((owners, tokens), 0) == shift * PLANE + mate, 1.0, 0.0)
    rank = jnp.sum(near * before(near), axis=0, keepdims=True).astype(i32)
    rest = rank >= DIRECT
    by_shift = jnp.where((iota((ZS, tokens), 0) == shift) & rest, 1.0, 0.0)
    order = jnp.sum(by_shift * before(by_shift), axis=0, keepdims=True).astype(i32)
    late = rest & (order >= LIMIT)
    first = jnp.where(rest & (order < LIMIT), shift * LIMIT + order, -1)
    plan[0:1] = jnp.where(rest, -1, owner * DIRECT + rank)
    plan[1:2] = first
    plan[2:3] = jnp.where(late, owner * REST + rank - DIRECT, -1)
    plan[3:8] = jnp.zeros((5, tokens), i32)
    over = jnp.max(jnp.where(late, 1.0, 0.0), axis=1, keepdims=True)
    lane = iota((NOTE, tokens), 0)
    code = jnp.where(lane == 2 * rank, row >> 4, 0) + jnp.where(lane == 2 * rank + 1, row & 15, 0)
    labels = dot_t(near.astype(bf16), code.astype(f32).astype(bf16))
    way = jnp.where(lane == ROUTE, mate * REST + (rank - DIRECT) + 1, 0)
    moved = onehot(iota((ZS * LIMIT, tokens), 0) == first)
    ways = dot_t(moved, way.astype(f32).astype(bf16))
    flag = jnp.where(iota((owners, NOTE), 1) == FLAG, over, 0.0)
    note[...] = (labels + ways + flag).astype(bf16)


def pair_weight(clen, rlen, clogp, rlogp, ref):
    length = clogp.shape[1]
    positions = iota((1, length), 1)
    chosen_mask = (positions >= length - clen).astype(f32)
    rejected_mask = (positions >= length - rlen).astype(f32)
    chosen = jnp.sum(chosen_mask * clogp[...], axis=1, keepdims=True)
    rejected = jnp.sum(rejected_mask * rlogp[...], axis=1, keepdims=True)
    margin = BETA * ((chosen - ref[0]) - (rejected - ref[1]))
    return BETA * (1.0 / (1.0 + jnp.exp(margin)))


def weighted(weight, cg, rg, rows):
    half = cg.shape[1]
    rows[:half] = (-weight[0:1, 0:1] * cg[0].astype(f32)).astype(bf16)
    rows[half:] = (weight[0:1, 0:1] * rg[0].astype(f32)).astype(bf16)


def first_kernel(cid, rid, lengths, clogp, rlogp, ref, cg, rg, *refs, row_count):
    outs = refs[:ZS]
    plan, weight, note, pick, rows, arrival = refs[ZS:]
    step = pl.program_id(0)
    last = pl.num_programs(0) - 1
    half = cg.shape[1]
    few = rows.shape[0]

    def fetches(n):
        columns = pl.ds(n * WIDE, WIDE)
        return [
            pltpu.make_async_copy(
                grads.at[0, :, columns], rows.at[n, pl.ds(i * half, half)], arrival.at[n, i]
            )
            for i, grads in enumerate((cg, rg))
        ]

    @pl.when(step == 0)
    def _():
        for n in range(few):
            for fetch in fetches(n):
                fetch.start()
        route(cid, rid, plan, note, row_count)
        weight[...] = jnp.broadcast_to(
            pair_weight(lengths[0], lengths[1], clogp, rlogp, ref), weight.shape
        )
        pick[...] = onehot(iota(pick.shape, 0) == plan[1:2])

    @pl.when(step < last)
    def _():
        for fetch in fetches(step):
            fetch.wait()
        scale = weight[0:1, 0:1]
        moved = dot(pick[:, :half], rows[step, :half]) * -scale
        moved += dot(pick[:, half:], rows[step, half:]) * scale
        moved = moved.astype(bf16)
        for d in range(ZS):
            outs[d][...] = moved[d * LIMIT : d * LIMIT + LIMIT]

    @pl.when(step == last)
    def _():
        for d in range(ZS):
            outs[d][:, :NOTE] = note[d * LIMIT : d * LIMIT + LIMIT]


def direct_kernel(plan, weight, cg, rg, out, rows, pick, wide, *, kind):
    step = pl.program_id(0)

    @pl.when(step == 0)
    def _():
        pick[...] = onehot(iota(pick.shape, 0) == plan[kind : kind + 1])

    weighted(weight, cg, rg, rows)
    width = out.shape[2]
    slots = pick.shape[0]
    moved = dot(pick[...], rows[...])
    for u in range(UNITS):
        wide[pl.ds(u, slots, stride=UNITS), :] = moved[:, u * width : (u + 1) * width]
    out[...] = wide[...].astype(bf16).reshape(out.shape)


def turned(turn, swap, place):
    y = (turn + place[3]) & (YS - 1)
    core = (swap + place[2]) & (CORES - 1)
    x = (turn // YS + place[1]) & (XS - 1)
    return (x * CORES + core) * YS + y


def second_kernel(*refs):
    place = here()
    arrived = refs[:ZS]
    notes = refs[ZS : 2 * ZS]
    outs = refs[2 * ZS : 2 * ZS + TURNS]
    pick, spread = refs[2 * ZS + TURNS :]
    step = pl.program_id(0)
    last = pl.num_programs(0) - 1
    each = ZS * REST
    both = CORES * each

    @pl.when(step == 0)
    def _():
        note = jnp.concatenate([n[...] for n in notes], axis=0).astype(f32)
        blocks = [jnp.transpose(note[b : b + 128]) for b in range(0, ZS * LIMIT, 128)]
        way = jnp.concatenate(blocks, axis=1)[ROUTE : ROUTE + 1].astype(i32)
        out_row = iota(pick.shape, 0)
        in_row = iota(pick.shape, 1)
        mate = turned(out_row // both, out_row // each, place)
        shift = (out_row // REST) & (ZS - 1)
        wanted = mate * REST + (out_row & (REST - 1)) + 1
        pick[...] = onehot((in_row // LIMIT == shift) & (way == wanted))
        spread[...] = onehot(in_row == shift * PLANE + mate)

    @pl.when(step < last)
    def _():
        rows = jnp.concatenate([a[...] for a in arrived], axis=0)
        moved = dot(pick[...], rows).astype(bf16)
        for e in range(TURNS):
            outs[e][...] = moved[e * both : e * both + both]

    @pl.when(step == last)
    def _():
        note = jnp.concatenate([n[...] for n in notes], axis=0)
        moved = dot(spread[...], note).astype(bf16)
        for e in range(TURNS):
            outs[e][:, :NOTE] = moved[e * both : e * both + both]


def stack_kernel(*refs):
    out = refs[-1]
    for i, part in enumerate(refs[:-1]):
        out[i * part.shape[0] : (i + 1) * part.shape[0]] = part[...]


def collect_kernel(*refs):
    place = here()
    parts = refs[: TURNS + 1]
    notes = refs[TURNS + 1 : 2 * TURNS + 2]
    rows, near, far, late, flag = refs[2 * TURNS + 2 :]
    each = ZS * REST
    count = PLANE * each
    owners = PLANE * ZS
    start = 0
    for part in parts:
        rows[start : start + part.shape[0]] = part[...]
        start += part.shape[0]

    @pl.when(pl.program_id(0) == 0)
    def _():
        note = jnp.concatenate([n[...] for n in notes], axis=0)
        wide = note.astype(f32)
        across = jnp.concatenate(
            [jnp.transpose(wide[b : b + 128]) for b in range(0, count, 128)], axis=1
        )
        flag[0] = jnp.max(across[FLAG : FLAG + 1]).astype(i32)

        def joined(across, ranks):
            which = iota((1, across.shape[1]), 1) % len(ranks)
            found = jnp.zeros(which.shape, f32)
            for i, rank in enumerate(ranks):
                high = across[2 * rank : 2 * rank + 1]
                low = across[2 * rank + 1 : 2 * rank + 2]
                found = found + jnp.where(which == i, 16.0 * high + low, 0.0)
            return found.astype(i32)

        straight = range(DIRECT)
        others = range(DIRECT, CAP)
        far[...] = joined(across, others)
        source = iota((owners, count), 0)
        item = iota((owners, count), 1)
        turn = item // each
        y = (place[3] - turn) & (YS - 1)
        x = (place[1] - turn // YS) & (XS - 1)
        core = (place[2] - turn // TURNS) & (CORES - 1)
        z = (place[0] - item // REST) & (ZS - 1)
        match = (source == ((x * CORES + core) * YS + y) * ZS + z) & ((item & (REST - 1)) == 0)
        by_source = dot(onehot(match), note).astype(bf16)
        for out, ranks in ((near, straight), (late, others)):
            places = owners * len(ranks)
            grow = onehot(iota((owners, places), 1) // len(ranks) == iota((owners, places), 0))
            grown = lax.dot_general(
                by_source, grow, (((0,), (0,)), ((), ())), preferred_element_type=f32
            )
            out[...] = joined(grown, ranks)


def finish_kernel(*refs, tiled):
    labels = refs[: tiled + 1]
    packed = refs[tiled + 1 : 2 * tiled + 1]
    rest = refs[2 * tiled + 1]
    out, pick, *scratch = refs[2 * tiled + 2 : 2 * tiled + 8]
    *blocks, others, arrival = refs[2 * tiled + 8 :]
    step = pl.program_id(0)

    def fetches(n):
        pairs = []
        for source, block in zip(packed, blocks):
            tall = block.shape[2]
            pairs.append((source.at[:, pl.ds(n * tall, tall)], block.at[n]))
        pairs.append((rest.at[:, pl.ds(n * STEP, STEP)], others.at[n]))
        return [
            pltpu.make_async_copy(source, target, arrival.at[n, i])
            for i, (source, target) in enumerate(pairs)
        ]

    @pl.when(step == 0)
    def _():
        for n in range(others.shape[0]):
            for fetch in fetches(n):
                fetch.start()
        start = 0
        for label in labels:
            size = label.shape[1]
            part = pick.at[:, start : start + size]
            part[...] = onehot(iota(part.shape, 0) == label[...])
            start += size

    for fetch in fetches(step):
        fetch.wait()
    total = dot(pick[:, -rest.shape[0] :], others[step])
    start = 0
    for block in blocks:
        _, count, tall, width = block.shape
        piece = CHUNK * UNITS // tall
        for first in range(0, count, piece):
            side = 2 * (start // CHUNK % 2)
            wide, rows = scratch[side : side + 2]
            wide[...] = block[step, first : first + piece].astype(f32).reshape(wide.shape)
            for u in range(UNITS):
                unit = wide[pl.ds(u, CHUNK, stride=UNITS), :].astype(bf16)
                rows[:, u * width : (u + 1) * width] = unit
            total += dot(pick[:, start : start + CHUNK], rows[...])
            start += CHUNK
    out[...] = total[: out.shape[0]].astype(bf16)


def shifted(dx, dcore, dy, dz):
    def at(x, core, y, z):
        return ((x % XS * CORES + core % CORES) * YS + y % YS) * ZS + z % ZS

    return [
        (at(x, core, y, z), at(x + dx, core + dcore, y + dy, z + dz))
        for x in range(XS)
        for core in range(CORES)
        for y in range(YS)
        for z in range(ZS)
    ]


def whole(*shape):
    return pl.BlockSpec(shape, lambda *_: (0,) * len(shape))


def local(cid, rid, clen, rlen, clogp, rlogp, ref, cg, rg):
    length, features = cg.shape[1:]
    tokens = 2 * length
    owners = PLANE * ZS
    row_count = VOCAB // owners
    axes = ("grp", "dp")
    smem = pl.BlockSpec(memory_space=pltpu.SMEM)
    columns = features + NOTE
    steps = features // STEP
    width = STEP // UNITS
    each = ZS * REST
    padded = (row_count + 15) // 16 * 16

    few = features // WIDE
    *first, plan, weight = pl.pallas_call(
        functools.partial(first_kernel, row_count=row_count),
        out_shape=[jax.ShapeDtypeStruct((LIMIT, columns), bf16)] * ZS
        + [jax.ShapeDtypeStruct((8, tokens), i32), jax.ShapeDtypeStruct((8, 128), f32)],
        grid=(few + 1,),
        in_specs=[whole(1, length)] * 2
        + [smem]
        + [whole(1, length)] * 2
        + [smem] + [pl.BlockSpec(memory_space=pl.ANY)] * 2,
        out_specs=[pl.BlockSpec((LIMIT, WIDE), lambda n: (0, n))] * ZS
        + [whole(8, tokens), whole(8, 128)],
        scratch_shapes=[
            pltpu.VMEM((owners, NOTE), bf16),
            pltpu.VMEM((ZS * LIMIT, tokens), bf16),
            pltpu.VMEM((few, tokens, WIDE), bf16),
            pltpu.SemaphoreType.DMA((few, 2)),
        ],
        name="first",
    )(
        cid,
        rid,
        jnp.concatenate([clen, rlen]),
        clogp,
        rlogp,
        ref.reshape(2),
        cg,
        rg,
    )
    hopped = list(first)
    for d in WAYS:
        hopped[d] = lax.ppermute(first[d], axes, shifted(0, 0, 0, d))

    def direct(kind, count):
        slots = owners * count
        sent = pl.pallas_call(
            functools.partial(direct_kernel, kind=kind),
            out_shape=jax.ShapeDtypeStruct((owners, steps * count * UNITS, width), bf16),
            grid=(steps,),
            in_specs=[
                whole(8, tokens),
                whole(8, 128),
                pl.BlockSpec((1, length, STEP), lambda n: (0, 0, n)),
                pl.BlockSpec((1, length, STEP), lambda n: (0, 0, n)),
            ],
            out_specs=pl.BlockSpec((owners, count * UNITS, width), lambda n: (0, n, 0)),
            scratch_shapes=[
                pltpu.VMEM((tokens, STEP), bf16),
                pltpu.VMEM((slots, tokens), bf16),
                pltpu.VMEM((slots * UNITS, width), f32),
            ],
            name="direct",
        )(plan, weight, cg, rg)
        return lax.all_to_all(sent, axes, split_axis=0, concat_axis=0, tiled=True)

    arrived = direct(0, DIRECT)

    both = CORES * each
    here_part = [pl.BlockSpec((LIMIT, WIDE), lambda n: (0, jnp.minimum(n, few - 1)))] * ZS
    here_note = [pl.BlockSpec((LIMIT, NOTE), lambda n: (0, features // NOTE))] * ZS
    second = pl.pallas_call(
        second_kernel,
        out_shape=[jax.ShapeDtypeStruct((both, columns), bf16)] * TURNS,
        grid=(few + 1,),
        in_specs=here_part + here_note,
        out_specs=[pl.BlockSpec((both, WIDE), lambda n: (0, n))] * TURNS,
        scratch_shapes=[
            pltpu.VMEM((PLANE * each, ZS * LIMIT), bf16),
            pltpu.VMEM((PLANE * each, ZS * LIMIT), bf16),
        ],
        name="second",
    )(*hopped, *hopped)
    turns = [second[0]] + [
        lax.ppermute(second[e], axes, shifted(e // YS, 0, e % YS, 0)) for e in range(1, TURNS)
    ]
    swap = pl.pallas_call(
        stack_kernel,
        out_shape=jax.ShapeDtypeStruct((TURNS * each, columns), bf16),
        grid=(few + 1,),
        in_specs=[pl.BlockSpec((each, WIDE), lambda n: (1, n))] * TURNS,
        out_specs=pl.BlockSpec((TURNS * each, WIDE), lambda n: (0, n)),
        name="stack",
    )(*turns)
    swap = lax.ppermute(swap, axes, shifted(0, 1, 0, 0))

    rest, near, far, late, flag = pl.pallas_call(
        collect_kernel,
        out_shape=[
            jax.ShapeDtypeStruct((PLANE * each, features), bf16),
            jax.ShapeDtypeStruct((1, owners * DIRECT), i32),
            jax.ShapeDtypeStruct((1, PLANE * each), i32),
            jax.ShapeDtypeStruct((1, owners * REST), i32),
            jax.ShapeDtypeStruct((1,), i32),
        ],
        grid=(few,),
        in_specs=[pl.BlockSpec((each, WIDE), lambda n: (0, n))] * TURNS
        + [pl.BlockSpec((TURNS * each, WIDE), lambda n: (0, n))]
        + [pl.BlockSpec((each, NOTE), lambda n: (0, features // NOTE))] * TURNS
        + [pl.BlockSpec((TURNS * each, NOTE), lambda n: (0, features // NOTE))],
        out_specs=[
            pl.BlockSpec((PLANE * each, WIDE), lambda n: (0, n)),
            whole(1, owners * DIRECT),
            whole(1, PLANE * each),
            whole(1, owners * REST),
            smem,
        ],
        name="collect",
    )(*turns, swap, *turns, swap)

    def finish(labels, packed):
        count = sum(label.shape[1] for label in labels)
        return pl.pallas_call(
            functools.partial(finish_kernel, tiled=len(packed)),
            out_shape=jax.ShapeDtypeStruct((row_count, features), bf16),
            grid=(steps,),
            in_specs=[whole(*label.shape) for label in labels]
            + [pl.BlockSpec(memory_space=pl.ANY)] * (len(packed) + 1),
            out_specs=pl.BlockSpec((row_count, STEP), lambda n: (0, n)),
            scratch_shapes=[pltpu.VMEM((padded, count), bf16)]
            + [
                pltpu.VMEM((CHUNK * UNITS, width), f32),
                pltpu.VMEM((CHUNK, STEP), bf16),
            ]
            * 2
            + [
                pltpu.VMEM((steps, owners, block.shape[1] // steps, width), bf16)
                for block in packed
            ]
            + [
                pltpu.VMEM((steps, PLANE * each, STEP), bf16),
                pltpu.SemaphoreType.DMA((steps, len(packed) + 1)),
            ],
            name="finish",
        )(*labels, *packed, rest)

    return lax.cond(
        flag[0] > 0,
        lambda: finish([near, late, far], [arrived, direct(2, REST)]),
        lambda: finish([near, far], [arrived]),
    )


def solution(mesh):
    return jax.shard_map(
        local,
        mesh=mesh,
        in_specs=(
            P(("grp", "dp"), None),
            P(("grp", "dp"), None),
            P(("grp", "dp")),
            P(("grp", "dp")),
            P(("grp", "dp"), None),
            P(("grp", "dp"), None),
            P(None, ("grp", "dp")),
            P(("grp", "dp"), None, None),
            P(("grp", "dp"), None, None),
        ),
        out_specs=P(("grp", "dp"), None),
        check_vma=False,
    )
```

```python
import functools

import jax
import jax.numpy as jnp
from jax import lax
from jax.experimental import pallas as pl
from jax.experimental.pallas import tpu as pltpu
from jax.sharding import PartitionSpec as P


VOCAB = 128256
BETA = 0.1
XS, CORES, YS, ZS = 4, 2, 4, 8
PLANE = XS * CORES * YS
CAP = 6
DIRECT = 4
REST = CAP - DIRECT
LIMIT = 32
UNITS = 4
NOTE = 128
FLAG, ROUTE = 12, 13
STEP = 512
WIDE = 1024
CHUNK = 512
WAYS = sorted(range(1, ZS), key=lambda d: -min(d, ZS - d))
TURNS = XS * YS

bf16 = jnp.bfloat16
f32 = jnp.float32
i32 = jnp.int32


def iota(shape, dim):
    return lax.broadcasted_iota(i32, shape, dim)


def onehot(hit):
    return jnp.where(hit, 1.0, 0.0).astype(bf16)


def dot(a, b):
    return jnp.dot(a, b, preferred_element_type=f32)


def dot_t(a, b):
    return lax.dot_general(a, b, (((1,), (1,)), ((), ())), preferred_element_type=f32)


def before(hits):
    tokens = hits.shape[1]
    block = 256
    earlier = onehot(iota((block, block), 0) < iota((block, block), 1))
    carry = jnp.zeros((hits.shape[0], 1), f32)
    counts = []
    for b in range(0, tokens, block):
        piece = hits[:, b : b + block]
        counts.append(dot(piece.astype(bf16), earlier) + carry)
        carry = carry + jnp.sum(piece, axis=1, keepdims=True)
    return jnp.concatenate(counts, axis=1)


def here():
    grp = lax.axis_index("grp")
    dp = lax.axis_index("dp")
    return dp & (ZS - 1), grp // CORES, grp & (CORES - 1), dp // ZS


def route(cid, rid, plan, note, row_count):
    ids = jnp.concatenate([cid[...], rid[...]], axis=1)
    owner = jnp.floor((ids.astype(f32) + 0.5) * (1.0 / row_count)).astype(i32)
    row = ids - owner * row_count
    mate = owner // ZS
    shift = (owner - here()[0]) & (ZS - 1)
    tokens = ids.shape[1]
    owners = PLANE * ZS
    near = jnp.where(iota((owners, tokens), 0) == shift * PLANE + mate, 1.0, 0.0)
    rank = jnp.sum(near * before(near), axis=0, keepdims=True).astype(i32)
    rest = rank >= DIRECT
    by_shift = jnp.where((iota((ZS, tokens), 0) == shift) & rest, 1.0, 0.0)
    order = jnp.sum(by_shift * before(by_shift), axis=0, keepdims=True).astype(i32)
    late = rest & (order >= LIMIT)
    first = jnp.where(rest & (order < LIMIT), shift * LIMIT + order, -1)
    plan[0:1] = jnp.where(rest, -1, owner * DIRECT + rank)
    plan[1:2] = first
    plan[2:3] = jnp.where(late, owner * REST + rank - DIRECT, -1)
    plan[3:8] = jnp.zeros((5, tokens), i32)
    over = jnp.max(jnp.where(late, 1.0, 0.0), axis=1, keepdims=True)
    lane = iota((NOTE, tokens), 0)
    code = jnp.where(lane == 2 * rank, row >> 4, 0) + jnp.where(lane == 2 * rank + 1, row & 15, 0)
    labels = dot_t(near.astype(bf16), code.astype(f32).astype(bf16))
    way = jnp.where(lane == ROUTE, mate * REST + (rank - DIRECT) + 1, 0)
    moved = onehot(iota((ZS * LIMIT, tokens), 0) == first)
    ways = dot_t(moved, way.astype(f32).astype(bf16))
    flag = jnp.where(iota((owners, NOTE), 1) == FLAG, over, 0.0)
    note[...] = (labels + ways + flag).astype(bf16)


def pair_weight(clen, rlen, clogp, rlogp, ref):
    length = clogp.shape[1]
    positions = iota((1, length), 1)
    chosen_mask = (positions >= length - clen).astype(f32)
    rejected_mask = (positions >= length - rlen).astype(f32)
    chosen = jnp.sum(chosen_mask * clogp[...], axis=1, keepdims=True)
    rejected = jnp.sum(rejected_mask * rlogp[...], axis=1, keepdims=True)
    margin = BETA * ((chosen - ref[0]) - (rejected - ref[1]))
    return BETA * (1.0 / (1.0 + jnp.exp(margin)))


def weighted(weight, cg, rg, rows):
    half = cg.shape[1]
    rows[:half] = (-weight[0:1, 0:1] * cg[0].astype(f32)).astype(bf16)
    rows[half:] = (weight[0:1, 0:1] * rg[0].astype(f32)).astype(bf16)


def first_kernel(cid, rid, clen, rlen, clogp, rlogp, ref, cg, rg, *refs, row_count):
    outs = refs[:ZS]
    plan, weight, note, pick, rows, arrival = refs[ZS:]
    step = pl.program_id(0)
    last = pl.num_programs(0) - 1
    half = cg.shape[1]
    few = rows.shape[0]

    def fetches(n):
        columns = pl.ds(n * WIDE, WIDE)
        return [
            pltpu.make_async_copy(
                grads.at[0, :, columns], rows.at[n, pl.ds(i * half, half)], arrival.at[n, i]
            )
            for i, grads in enumerate((cg, rg))
        ]

    @pl.when(step == 0)
    def _():
        for n in range(few):
            for fetch in fetches(n):
                fetch.start()
        route(cid, rid, plan, note, row_count)
        weight[...] = jnp.broadcast_to(
            pair_weight(clen[0], rlen[0], clogp, rlogp, ref), weight.shape
        )
        pick[...] = onehot(iota(pick.shape, 0) == plan[1:2])

    @pl.when(step < last)
    def _():
        for fetch in fetches(step):
            fetch.wait()
        scale = weight[0:1, 0:1]
        moved = dot(pick[:, :half], rows[step, :half]) * -scale
        moved += dot(pick[:, half:], rows[step, half:]) * scale
        moved = moved.astype(bf16)
        for d in range(ZS):
            outs[d][...] = moved[d * LIMIT : d * LIMIT + LIMIT]

    @pl.when(step == last)
    def _():
        for d in range(ZS):
            outs[d][:, :NOTE] = note[d * LIMIT : d * LIMIT + LIMIT]


def direct_kernel(plan, weight, cg, rg, out, rows, pick, wide, *, kind):
    step = pl.program_id(0)

    @pl.when(step == 0)
    def _():
        pick[...] = onehot(iota(pick.shape, 0) == plan[kind : kind + 1])

    weighted(weight, cg, rg, rows)
    width = out.shape[2]
    slots = pick.shape[0]
    moved = dot(pick[...], rows[...])
    for u in range(UNITS):
        wide[pl.ds(u, slots, stride=UNITS), :] = moved[:, u * width : (u + 1) * width]
    out[...] = wide[...].astype(bf16).reshape(out.shape)


def turned(turn, swap, place):
    y = (turn + place[3]) & (YS - 1)
    core = (swap + place[2]) & (CORES - 1)
    x = (turn // YS + place[1]) & (XS - 1)
    return (x * CORES + core) * YS + y


def second_kernel(*refs):
    place = here()
    arrived = refs[:ZS]
    notes = refs[ZS : 2 * ZS]
    outs = refs[2 * ZS : 2 * ZS + TURNS]
    pick, spread = refs[2 * ZS + TURNS :]
    step = pl.program_id(0)
    last = pl.num_programs(0) - 1
    each = ZS * REST
    both = CORES * each

    @pl.when(step == 0)
    def _():
        note = jnp.concatenate([n[...] for n in notes], axis=0).astype(f32)
        blocks = [jnp.transpose(note[b : b + 128]) for b in range(0, ZS * LIMIT, 128)]
        way = jnp.concatenate(blocks, axis=1)[ROUTE : ROUTE + 1].astype(i32)
        out_row = iota(pick.shape, 0)
        in_row = iota(pick.shape, 1)
        mate = turned(out_row // both, out_row // each, place)
        shift = (out_row // REST) & (ZS - 1)
        wanted = mate * REST + (out_row & (REST - 1)) + 1
        pick[...] = onehot((in_row // LIMIT == shift) & (way == wanted))
        spread[...] = onehot(in_row == shift * PLANE + mate)

    @pl.when(step < last)
    def _():
        rows = jnp.concatenate([a[...] for a in arrived], axis=0)
        moved = dot(pick[...], rows).astype(bf16)
        for e in range(TURNS):
            outs[e][...] = moved[e * both : e * both + both]

    @pl.when(step == last)
    def _():
        note = jnp.concatenate([n[...] for n in notes], axis=0)
        moved = dot(spread[...], note).astype(bf16)
        for e in range(TURNS):
            outs[e][:, :NOTE] = moved[e * both : e * both + both]


def stack_kernel(*refs):
    out = refs[-1]
    for i, part in enumerate(refs[:-1]):
        out[i * part.shape[0] : (i + 1) * part.shape[0]] = part[...]


def collect_kernel(*refs):
    place = here()
    parts = refs[: TURNS + 1]
    notes = refs[TURNS + 1 : 2 * TURNS + 2]
    *rows, near, far, late, flag = refs[2 * TURNS + 2 :]
    each = ZS * REST
    count = PLANE * each
    owners = PLANE * ZS
    last = pl.num_programs(0) - 1
    for out, now in zip(rows, (pl.program_id(0) < last, pl.program_id(0) == last)):

        @pl.when(now)
        def _():
            start = 0
            for part in parts:
                out[start : start + part.shape[0]] = part[...]
                start += part.shape[0]

    @pl.when(pl.program_id(0) == 0)
    def _():
        note = jnp.concatenate([n[...] for n in notes], axis=0)
        wide = note.astype(f32)
        across = jnp.concatenate(
            [jnp.transpose(wide[b : b + 128]) for b in range(0, count, 128)], axis=1
        )
        flag[0] = jnp.max(across[FLAG : FLAG + 1]).astype(i32)

        def joined(across, ranks):
            which = iota((1, across.shape[1]), 1) % len(ranks)
            found = jnp.zeros(which.shape, f32)
            for i, rank in enumerate(ranks):
                high = across[2 * rank : 2 * rank + 1]
                low = across[2 * rank + 1 : 2 * rank + 2]
                found = found + jnp.where(which == i, 16.0 * high + low, 0.0)
            return found.astype(i32)

        straight = range(DIRECT)
        others = range(DIRECT, CAP)
        far[...] = joined(across, others)
        source = iota((owners, count), 0)
        item = iota((owners, count), 1)
        turn = item // each
        y = (place[3] - turn) & (YS - 1)
        x = (place[1] - turn // YS) & (XS - 1)
        core = (place[2] - turn // TURNS) & (CORES - 1)
        z = (place[0] - item // REST) & (ZS - 1)
        match = (source == ((x * CORES + core) * YS + y) * ZS + z) & ((item & (REST - 1)) == 0)
        by_source = dot(onehot(match), note).astype(bf16)
        for out, ranks in ((near, straight), (late, others)):
            places = owners * len(ranks)
            grow = onehot(iota((owners, places), 1) // len(ranks) == iota((owners, places), 0))
            grown = lax.dot_general(
                by_source, grow, (((0,), (0,)), ((), ())), preferred_element_type=f32
            )
            out[...] = joined(grown, ranks)


def finish_kernel(*refs, tiled):
    labels = refs[: tiled + 1]
    packed = refs[tiled + 1 : 2 * tiled + 1]
    rest = refs[2 * tiled + 1 : 2 * tiled + 3]
    out, pick, *scratch = refs[2 * tiled + 3 : 2 * tiled + 9]
    *blocks, others, arrival = refs[2 * tiled + 9 :]
    step = pl.program_id(0)
    split = rest[0].shape[1] // STEP

    def fetches(n, late):
        pairs = []
        for source, block in zip(packed, blocks):
            tall = block.shape[2]
            pairs.append((source.at[:, pl.ds(n * tall, tall)], block.at[n]))
        column = (n - split * late) * STEP
        pairs.append((rest[late].at[:, pl.ds(column, STEP)], others.at[n]))
        return [
            pltpu.make_async_copy(source, target, arrival.at[n, i])
            for i, (source, target) in enumerate(pairs)
        ]

    @pl.when(step == 0)
    def _():
        for n in range(others.shape[0]):
            for fetch in fetches(n, int(n >= split)):
                fetch.start()
        start = 0
        for label in labels:
            size = label.shape[1]
            part = pick.at[:, start : start + size]
            part[...] = onehot(iota(part.shape, 0) == label[...])
            start += size

    for late in range(2):

        @pl.when((step >= split) == bool(late))
        def _():
            for fetch in fetches(step, late):
                fetch.wait()

    total = dot(pick[:, -others.shape[1] :], others[step])
    start = 0
    for block in blocks:
        _, count, tall, width = block.shape
        piece = CHUNK * UNITS // tall
        for first in range(0, count, piece):
            side = 2 * (start // CHUNK % 2)
            wide, rows = scratch[side : side + 2]
            wide[...] = block[step, first : first + piece].astype(f32).reshape(wide.shape)
            for u in range(UNITS):
                unit = wide[pl.ds(u, CHUNK, stride=UNITS), :].astype(bf16)
                rows[:, u * width : (u + 1) * width] = unit
            total += dot(pick[:, start : start + CHUNK], rows[...])
            start += CHUNK
    out[...] = total[: out.shape[0]].astype(bf16)


def shifted(dx, dcore, dy, dz):
    def at(x, core, y, z):
        return ((x % XS * CORES + core % CORES) * YS + y % YS) * ZS + z % ZS

    return [
        (at(x, core, y, z), at(x + dx, core + dcore, y + dy, z + dz))
        for x in range(XS)
        for core in range(CORES)
        for y in range(YS)
        for z in range(ZS)
    ]


def whole(*shape):
    return pl.BlockSpec(shape, lambda *_: (0,) * len(shape))


def local(cid, rid, clen, rlen, clogp, rlogp, ref, cg, rg):
    length, features = cg.shape[1:]
    tokens = 2 * length
    owners = PLANE * ZS
    row_count = VOCAB // owners
    axes = ("grp", "dp")
    smem = pl.BlockSpec(memory_space=pltpu.SMEM)
    columns = features + NOTE
    steps = features // STEP
    width = STEP // UNITS
    each = ZS * REST
    padded = (row_count + 15) // 16 * 16

    few = features // WIDE
    *first, plan, weight = pl.pallas_call(
        functools.partial(first_kernel, row_count=row_count),
        out_shape=[jax.ShapeDtypeStruct((LIMIT, columns), bf16)] * ZS
        + [jax.ShapeDtypeStruct((8, tokens), i32), jax.ShapeDtypeStruct((8, 128), f32)],
        grid=(few + 1,),
        in_specs=[whole(1, length)] * 2
        + [smem] * 2
        + [whole(1, length)] * 2
        + [smem] + [pl.BlockSpec(memory_space=pl.ANY)] * 2,
        out_specs=[pl.BlockSpec((LIMIT, WIDE), lambda n: (0, n))] * ZS
        + [whole(8, tokens), whole(8, 128)],
        scratch_shapes=[
            pltpu.VMEM((owners, NOTE), bf16),
            pltpu.VMEM((ZS * LIMIT, tokens), bf16),
            pltpu.VMEM((few, tokens, WIDE), bf16),
            pltpu.SemaphoreType.DMA((few, 2)),
        ],
        name="first",
    )(
        cid,
        rid,
        clen,
        rlen,
        clogp,
        rlogp,
        ref.reshape(2),
        cg,
        rg,
    )
    hopped = list(first)
    for d in WAYS:
        hopped[d] = lax.ppermute(first[d], axes, shifted(0, 0, 0, d))

    def direct(kind, count):
        slots = owners * count
        sent = pl.pallas_call(
            functools.partial(direct_kernel, kind=kind),
            out_shape=jax.ShapeDtypeStruct((owners, steps * count * UNITS, width), bf16),
            grid=(steps,),
            in_specs=[
                whole(8, tokens),
                whole(8, 128),
                pl.BlockSpec((1, length, STEP), lambda n: (0, 0, n)),
                pl.BlockSpec((1, length, STEP), lambda n: (0, 0, n)),
            ],
            out_specs=pl.BlockSpec((owners, count * UNITS, width), lambda n: (0, n, 0)),
            scratch_shapes=[
                pltpu.VMEM((tokens, STEP), bf16),
                pltpu.VMEM((slots, tokens), bf16),
                pltpu.VMEM((slots * UNITS, width), f32),
            ],
            name="direct",
        )(plan, weight, cg, rg)
        return lax.all_to_all(sent, axes, split_axis=0, concat_axis=0, tiled=True)

    arrived = direct(0, DIRECT)

    both = CORES * each
    here_part = [pl.BlockSpec((LIMIT, WIDE), lambda n: (0, jnp.minimum(n, few - 1)))] * ZS
    here_note = [pl.BlockSpec((LIMIT, NOTE), lambda n: (0, features // NOTE))] * ZS
    second = pl.pallas_call(
        second_kernel,
        out_shape=[jax.ShapeDtypeStruct((both, columns), bf16)] * TURNS,
        grid=(few + 1,),
        in_specs=here_part + here_note,
        out_specs=[pl.BlockSpec((both, WIDE), lambda n: (0, n))] * TURNS,
        scratch_shapes=[
            pltpu.VMEM((PLANE * each, ZS * LIMIT), bf16),
            pltpu.VMEM((PLANE * each, ZS * LIMIT), bf16),
        ],
        name="second",
    )(*hopped, *hopped)
    turns = [second[0]] + [
        lax.ppermute(second[e], axes, shifted(e // YS, 0, e % YS, 0)) for e in range(1, TURNS)
    ]
    swap = pl.pallas_call(
        stack_kernel,
        out_shape=jax.ShapeDtypeStruct((TURNS * each, columns), bf16),
        grid=(few + 1,),
        in_specs=[pl.BlockSpec((each, WIDE), lambda n: (1, n))] * TURNS,
        out_specs=pl.BlockSpec((TURNS * each, WIDE), lambda n: (0, n)),
        name="stack",
    )(*turns)
    swap = lax.ppermute(swap, axes, shifted(0, 1, 0, 0))

    *rest, near, far, late, flag = pl.pallas_call(
        collect_kernel,
        out_shape=[
            jax.ShapeDtypeStruct((PLANE * each, features - WIDE), bf16),
            jax.ShapeDtypeStruct((PLANE * each, WIDE), bf16),
            jax.ShapeDtypeStruct((1, owners * DIRECT), i32),
            jax.ShapeDtypeStruct((1, PLANE * each), i32),
            jax.ShapeDtypeStruct((1, owners * REST), i32),
            jax.ShapeDtypeStruct((1,), i32),
        ],
        grid=(few,),
        in_specs=[pl.BlockSpec((each, WIDE), lambda n: (0, n))] * TURNS
        + [pl.BlockSpec((TURNS * each, WIDE), lambda n: (0, n))]
        + [pl.BlockSpec((each, NOTE), lambda n: (0, features // NOTE))] * TURNS
        + [pl.BlockSpec((TURNS * each, NOTE), lambda n: (0, features // NOTE))],
        out_specs=[
            pl.BlockSpec((PLANE * each, WIDE), lambda n: (0, jnp.minimum(n, few - 2))),
            whole(PLANE * each, WIDE),
            whole(1, owners * DIRECT),
            whole(1, PLANE * each),
            whole(1, owners * REST),
            smem,
        ],
        name="collect",
    )(*turns, swap, *turns, swap)

    def finish(labels, packed):
        count = sum(label.shape[1] for label in labels)
        return pl.pallas_call(
            functools.partial(finish_kernel, tiled=len(packed)),
            out_shape=jax.ShapeDtypeStruct((row_count, features), bf16),
            grid=(steps,),
            in_specs=[whole(*label.shape) for label in labels]
            + [pl.BlockSpec(memory_space=pl.ANY)] * (len(packed) + 2),
            out_specs=pl.BlockSpec((row_count, STEP), lambda n: (0, n)),
            scratch_shapes=[pltpu.VMEM((padded, count), bf16)]
            + [
                pltpu.VMEM((CHUNK * UNITS, width), f32),
                pltpu.VMEM((CHUNK, STEP), bf16),
            ]
            * 2
            + [
                pltpu.VMEM((steps, owners, block.shape[1] // steps, width), bf16)
                for block in packed
            ]
            + [
                pltpu.VMEM((steps, PLANE * each, STEP), bf16),
                pltpu.SemaphoreType.DMA((steps, len(packed) + 1)),
            ],
            name="finish",
        )(*labels, *packed, *rest)

    return lax.cond(
        flag[0] > 0,
        lambda: finish([near, late, far], [arrived, direct(2, REST)]),
        lambda: finish([near, far], [arrived]),
    )


def solution(mesh):
    return jax.shard_map(
        local,
        mesh=mesh,
        in_specs=(
            P(("grp", "dp"), None),
            P(("grp", "dp"), None),
            P(("grp", "dp")),
            P(("grp", "dp")),
            P(("grp", "dp"), None),
            P(("grp", "dp"), None),
            P(None, ("grp", "dp")),
            P(("grp", "dp"), None, None),
            P(("grp", "dp"), None, None),
        ),
        out_specs=P(("grp", "dp"), None),
        check_vma=False,
    )
```
